32 devices in a mesh: gx: 4 (over z), gy: 4 (over x, core), ens: 2 (over y).
Axes of the slice: x: 2, y: 2, z: 4, core: 2. Of those that a mesh axis runs over, the one named last changes fastest.
Arguments:
- state: float32 [128, 64, 512], P('ens', 'gy', 'gx'), may hold values from -6 to 6
- u_vel: float32 [64, 512], P('gy', 'gx'), may hold values from -0.4 to 0.4
- v_vel: float32 [64, 512], P('gy', 'gx'), may hold values from -0.4 to 0.4
- land: int32 [64, 512], P('gy', 'gx'), may hold values 0 or 1
- forcing: float32 [8, 64, 512], P(None, 'gy', 'gx'), may hold values from -3 to 3
- member_mode: int32 [128], P('ens'), may hold values from 0 to 7
- theta: float32 [128, 4], P('ens'), may hold values from -1 to 1
- obs_index: int32 [4, 4, 128], P('gy', 'gx'), may hold values from 0 to 2047
- obs_values: float32 [4, 4, 128], P('gy', 'gx'), may hold values from -6 to 6
- obs_sigma: float32 [4, 4, 128], P('gy', 'gx'), may hold values from 0.5 to 4
Outputs:
- final_state: float32 [128, 64, 512], P('ens', 'gy', 'gx')
- new_theta: float32 [128, 4], P('ens')
The draws below stay inside these ranges and needn't reach their ends.
All inputs are finite; a program needn't handle non-finite values. No bound on the sum of `land` on one device may be relied on, other than what follows from the above.
Results may differ from the reference program's by a relative error of at most 0.0003.
Values sent between devices are 32-bit elements; how exact they have to be, the bound alone decides.
A program may use at most 64 MiB of HBM per device.

```python
import math
import jax
import jax.numpy as jnp
from jax import lax

M = 128
P_SIZE = 4
K = 8
CX = 128
CY = 16
OBS_T = 128
STEPS = 4
NX = 512
NY = 64
N_GX = 4
N_GY = 4


def plant(entries, own_key, least, top_value):
    extent = entries.shape
    place = [jax.random.randint(jax.random.fold_in(own_key, axis), (), 0, extent[axis]) for axis in range(len(extent))]
    entries = entries.at[tuple(place)].set(least)
    longest = extent.index(max(extent))
    place[longest] = (place[longest] + 1) % extent[longest]
    return entries.at[tuple(place)].set(top_value)


def block_scale(stream_key, extent, cuts, low, largest):
    def one(dim, blocks):
        draws = jax.random.uniform(jax.random.fold_in(jax.random.fold_in(stream_key, 6), dim), (blocks,), jnp.float32, low / len(cuts), largest / len(cuts))
        return jnp.repeat(jnp.exp(draws), extent[dim] // blocks).reshape((-1,) + (1,) * (len(extent) - dim - 1))

    level = one(*cuts[0])
    for cut in cuts[1:]:
        level = level * one(*cut)
    return level


def scatter_about(key, dims, width, bound, shards=(), kind=jnp.bfloat16):
    gain = block_scale(key, dims, shards, -0.22, 0.18) if shards else 1.0
    drawn = jax.random.normal(key, dims, jnp.float32) * width * gain
    return jnp.minimum(jnp.maximum(drawn, -bound), bound).astype(kind)


def setup_inputs(seed: int = 0) -> dict:
    streams_of = jax.random.split(jax.random.key(seed), 11)
    return {
        "state": scatter_about(streams_of[0], (M, NY, NX), 1.0, 6.0, ((0, 2), (1, 4), (2, 4)), jnp.float32),
        "u_vel": jnp.clip(jax.random.uniform(streams_of[1], (NY, NX), jnp.float32, -0.4, 0.4) * block_scale(streams_of[1], (NY, NX), ((0, 4), (1, 4)), -0.4, 0.0), -0.4, 0.4),
        "v_vel": jnp.clip(jax.random.uniform(streams_of[2], (NY, NX), jnp.float32, -0.4, 0.4) * block_scale(streams_of[2], (NY, NX), ((0, 4), (1, 4)), -0.4, 0.0), -0.4, 0.4),
        "land": plant((jax.random.randint(streams_of[3], (NY, NX), 0, 8) < 1).astype(jnp.int32), jax.random.fold_in(streams_of[3], 1), 0, 1),
        "forcing": scatter_about(streams_of[4], (K, NY, NX), 0.5, 3.0, ((1, 4), (2, 4)), jnp.float32),
        "member_mode": plant(jax.random.randint(streams_of[5], (M,), 0, K), jax.random.fold_in(streams_of[5], 1), 0, K - 1).astype(jnp.int32),
        "theta": jnp.clip(jax.random.uniform(streams_of[6], (M, P_SIZE), jnp.float32, -1.0, 1.0) * block_scale(streams_of[6], (M, P_SIZE), ((0, 2),), -0.4, 0.0), -1.0, 1.0),
        "obs_index": plant(jax.random.randint(streams_of[7], (N_GY, N_GX, OBS_T), 0, CY * CX), jax.random.fold_in(streams_of[7], 1), 0, (CY * CX) - 1).astype(jnp.int32),
        "obs_values": scatter_about(streams_of[8], (N_GY, N_GX, OBS_T), 1.0, 6.0, ((0, 4), (1, 4)), jnp.float32),
        "obs_sigma": jnp.clip(jnp.exp(math.log(4.0) - 2.0794415 * jax.random.uniform(streams_of[9], (N_GY, N_GX, OBS_T), jnp.float32) ** block_scale(streams_of[9], (N_GY, N_GX, OBS_T), ((0, 4), (1, 4)), -0.2, 0.2)), 0.5, 4.0),
    }


def laplace(field):
    upper = jnp.pad(field[1:], ((0, 1), (0, 0)))
    lower = jnp.pad(field[:-1], ((1, 0), (0, 0)))
    return upper + lower + jnp.roll(field, -1, 1) + jnp.roll(field, 1, 1) - 4.0 * field

def reference(state, u_vel, v_vel, land, forcing, member_mode, theta, obs_index, obs_values, obs_sigma):
    ocean = (1 - land).astype(jnp.float32)
    tile_rows = jnp.arange(N_GY, dtype=jnp.int32)[:, None, None] * CY
    tile_cols = jnp.arange(N_GX, dtype=jnp.int32)[None, :, None] * CX
    site_rows = (tile_rows + obs_index // CX).reshape(-1)
    site_cols = (tile_cols + obs_index % CX).reshape(-1)

    def advance(member_data):
        field, mode, params = member_data
        diffuse = 0.05 * (1.0 + 0.5 * jnp.tanh(params[0]))
        hyper = 0.005 * (1.0 + 0.5 * jnp.tanh(params[1]))
        damping = 0.05 * (1.0 + 0.5 * jnp.tanh(params[2]))
        forced = params[3] * forcing[mode]
        for step_index in range(STEPS):
            lap_field = laplace(field)
            biharm = laplace(lap_field)
            upper = jnp.pad(field[1:], ((0, 1), (0, 0)))
            lower = jnp.pad(field[:-1], ((1, 0), (0, 0)))
            grad_x = 0.5 * (jnp.roll(field, -1, 1) - jnp.roll(field, 1, 1))
            grad_y = 0.5 * (upper - lower)
            tend = diffuse * lap_field - hyper * biharm - damping * field + forced - (u_vel * grad_x + v_vel * grad_y)
            field = (field + tend) * ocean
        return (field, field[site_rows, site_cols])
    final_state, observed = lax.map(advance, (state, member_mode, theta))
    sigma = obs_sigma.reshape(-1)
    target = obs_values.reshape(-1)
    anomaly = (observed - jnp.mean(observed, 0)) / sigma
    misfit = (target - observed) / sigma
    gram = jnp.dot(anomaly.astype(jnp.float32), anomaly.T.astype(jnp.float32), preferred_element_type=jnp.float32, precision=lax.Precision.HIGHEST)
    cross = jnp.dot(anomaly.astype(jnp.float32), misfit.T.astype(jnp.float32), preferred_element_type=jnp.float32, precision=lax.Precision.HIGHEST)
    system = gram + (M - 1) * jnp.eye(M, dtype=jnp.float32)
    weights = jnp.linalg.solve(system, cross)
    spread = theta - jnp.mean(theta, 0)
    new_theta = theta + jnp.dot(weights.T.astype(jnp.float32), spread.astype(jnp.float32), preferred_element_type=jnp.float32, precision=lax.Precision.HIGHEST)
    return (final_state, new_theta)
```

```python
import functools
import jax
import jax.numpy as jnp
from jax import lax
from jax.experimental import pallas as pl
from jax.experimental.pallas import tpu as pltpu
from jax.sharding import PartitionSpec as P

STEPS = 4
DEPTH = 2 * STEPS
F32 = jnp.float32
I32 = jnp.int32
VM = pltpu.VMEM
MESH = pl.DeviceIdType.MESH
HIGH = lax.Precision.HIGHEST


def vspec():
    return pl.BlockSpec(memory_space=pltpu.VMEM)


def anyspec():
    return pl.BlockSpec(memory_space=pl.ANY)


def flat(ref):
    return ref.reshape(ref.shape[0] * ref.shape[1], ref.shape[2])


def rdma(src, dst, send, recv, dev):
    return pltpu.make_async_remote_copy(src_ref=src, dst_ref=dst, send_sem=send, recv_sem=recv,
                                        device_id=dev, device_id_type=MESH)


def step_kernel(n_gx, n_gy, n_ens, reduce_here,
                state_ref, forcing_ref, u_ref, v_ref, land_ref, mode_in, theta_in, index_in, val_in, sig_in,
                final_ref, full_ref, c_ref, th_ref,
                q_lo, q_hi, f_lo, f_hi, land_b, mode_ref, theta_ref, index_ref, val_ref, sig_ref,
                qt_ref, qb_ref, ft_ref, fb_ref, pack, mid_ref, top_ref, bot_ref,
                Q, L, FO, US, H, LH, FH, UH, TH, out_ref,
                obs_ref, obs_all, part, rs, c_own, cs,
                load_sem, store_sem, row_send, row_recv, gx_send, gx_recv, gy_send, gy_recv,
                ens_send, ens_recv, rs_send, rs_recv, cs_send, cs_recv, ag_send, ag_recv):
    gx, gy, ens = lax.axis_index("gx"), lax.axis_index("gy"), lax.axis_index("ens")
    right, left = lax.rem(gx + 1, n_gx), lax.rem(gx + n_gx - 1, n_gx)
    has_up, has_down = gy > 0, gy < n_gy - 1
    up, down = jnp.maximum(gy - 1, 0), jnp.minimum(gy + 1, n_gy - 1)
    members, rows, cols = state_ref.shape
    patterns = forcing_ref.shape[0]
    fields = patterns + 3
    n_rows = rows + 2 * DEPTH
    n = n_gx * n_gy
    me = gy * n_gx + gx
    peers = [lax.rem(me + o, n) for o in range(1, n)] if reduce_here else []
    where = [{"gx": lax.rem(p, n_gx), "gy": lax.div(p, n_gx)} for p in peers]
    others = [lax.rem(ens + o, n_ens) for o in range(1, n_ens)]

    barrier = pltpu.get_barrier_semaphore()
    for p in others:
        pl.semaphore_signal(barrier, inc=1, device_id={"ens": p}, device_id_type=MESH)
    if reduce_here:
        for p in where:
            pl.semaphore_signal(barrier, inc=1, device_id=p, device_id_type=MESH)
        expected = len(others) + len(where)
    else:
        pl.semaphore_signal(barrier, inc=1, device_id={"gx": right}, device_id_type=MESH)
        pl.semaphore_signal(barrier, inc=1, device_id={"gx": left}, device_id_type=MESH)

        @pl.when(has_up)
        def _():
            pl.semaphore_signal(barrier, inc=1, device_id={"gy": up}, device_id_type=MESH)

        @pl.when(has_down)
        def _():
            pl.semaphore_signal(barrier, inc=1, device_id={"gy": down}, device_id_type=MESH)
        expected = len(others) + 2 + has_up.astype(I32) + has_down.astype(I32)

    pairs = [(state_ref.at[:, 0:DEPTH, :], q_lo), (state_ref.at[:, rows - DEPTH:, :], q_hi)]
    for h, dst in ((0, f_lo), (rows - DEPTH, f_hi)):
        pairs += [(forcing_ref.at[:, h:h + DEPTH, :], dst.at[0:patterns]),
                  (u_ref.at[h:h + DEPTH, :], dst.at[patterns]), (v_ref.at[h:h + DEPTH, :], dst.at[patterns + 1])]
    pairs += [(land_ref, land_b), (mode_in, mode_ref), (theta_in, theta_ref), (index_in, index_ref),
              (val_in, val_ref), (sig_in, sig_ref)]
    loads = [pltpu.make_async_copy(s, d, load_sem.at[k]) for k, (s, d) in enumerate(pairs)]
    for c in loads:
        c.start()

    shape = (8, cols)
    lane = lax.broadcasted_iota(I32, shape, 1)
    sub = lax.broadcasted_iota(I32, shape, 0)
    half_ok = jnp.where(lane < cols // 2, has_down.astype(I32), has_up.astype(I32)) > 0
    bits = {k: jnp.bitwise_and(lane, k) != 0 for k in (1, 2, 4)}

    def roll(x, k):
        return pltpu.roll(x, k % cols, 1)

    def butterfly(xs):
        xs = list(xs)
        for k in (1, 2, 4):
            for v in range(8):
                if not v & k:
                    x, y = xs[v], xs[v | k]
                    xs[v] = jnp.where(bits[k], roll(y, k), x)
                    xs[v | k] = jnp.where(bits[k], y, roll(x, -k))
        return xs

    def gather(x, idx, axis):
        return jnp.take_along_axis(x, idx, axis=axis, mode="promise_in_bounds")

    for c in loads:
        c.wait()
    for h, dst in ((0, f_lo), (rows - DEPTH, f_hi)):
        dst[patterns + 2] = (1 - land_b[h:h + DEPTH, :]).astype(F32)
        dst[fields:] = jnp.zeros((dst.shape[0] - fields, DEPTH, cols), F32)

    pl.semaphore_wait(barrier, expected)

    downs = [rdma(q_hi, qt_ref, row_send.at[0], row_recv.at[0], {"gy": down}),
             rdma(f_hi.at[0:fields], ft_ref.at[0:fields], row_send.at[1], row_recv.at[1], {"gy": down})]
    ups = [rdma(q_lo, qb_ref, row_send.at[2], row_recv.at[2], {"gy": up}),
           rdma(f_lo.at[0:fields], fb_ref.at[0:fields], row_send.at[3], row_recv.at[3], {"gy": up})]
    strip_down = rdma(mid_ref, top_ref, gy_send.at[0], gy_recv.at[0], {"gy": down})
    strip_up = rdma(mid_ref, bot_ref, gy_send.at[1], gy_recv.at[1], {"gy": up})

    @pl.when(has_down)
    def _():
        for c in downs:
            c.start()

    @pl.when(has_up)
    def _():
        for c in ups:
            c.start()

    def pack_from(lo_ref, hi_ref, base):
        for g in range(lo_ref.shape[0] // 8):
            lo = jnp.zeros(shape, F32)
            hi = jnp.zeros(shape, F32)
            for r in range(rows):
                ref = flat(lo_ref if r < DEPTH else hi_ref)
                val = ref[pl.ds(g * 8 * DEPTH + r % DEPTH, 8, stride=DEPTH), :]
                mine = (lane // DEPTH) == r
                hi = jnp.where(mine, roll(val, r * DEPTH + DEPTH), hi)
                lo = jnp.where(mine, roll(val, r * DEPTH), lo)
            pack[0, base + g * 8:base + g * 8 + 8, :] = hi
            pack[1, base + g * 8:base + g * 8 + 8, :] = lo

    pack_from(q_lo, q_hi, 0)
    pack_from(f_lo, f_hi, members)
    to_right = rdma(pack.at[0], mid_ref.at[0], gx_send.at[0], gx_recv.at[0], {"gx": right})
    to_left = rdma(pack.at[1], mid_ref.at[1], gx_send.at[1], gx_recv.at[1], {"gx": left})
    to_right.start()
    to_left.start()

    TH[...] = jnp.zeros_like(TH)
    TH[0:theta_ref.shape[0], 0:members] = theta_ref[...]
    slot = sub * 8 + jnp.bitwise_and(lane, 7)
    par = [gather(jnp.broadcast_to(TH[k:k + 1, :], shape), slot, 1) for k in range(4)]
    diffuse = 0.05 * (1.0 + 0.5 * jnp.tanh(par[0]))
    hyper = 0.005 * (1.0 + 0.5 * jnp.tanh(par[1]))
    keep = 1.0 - 0.05 * (1.0 + 0.5 * jnp.tanh(par[2]))
    gain = par[3]
    mrow = jnp.concatenate([mode_ref[...], jnp.zeros((1, cols - members), I32)], axis=1)
    pattern_of = gather(jnp.broadcast_to(mrow, shape), slot, 1)
    block0 = lane - jnp.bitwise_and(lane, 7)

    def spread(x):
        return [gather(x, block0 + c, 1) for c in range(8)]

    def forced(x):
        return [gain * gather(y, pattern_of, 0) for y in spread(x)]

    def enter(ref, fr, base, ok):
        ref, fr = flat(ref), flat(fr)

        def keep_in(x):
            return x if ok is None else jnp.where(ok, x, 0.0)

        for k in range(DEPTH):
            ys = butterfly([keep_in(ref[pl.ds(v * DEPTH + k, 8, stride=8 * DEPTH), :]) for v in range(8)])
            zs = forced(keep_in(fr[pl.ds(k, 8, stride=DEPTH), :]))
            for c in range(8):
                Q[0, base + k, c] = ys[c]
                FO[base + k, c] = zs[c]
        for f in range(3):
            x = keep_in(fr[(patterns + f) * DEPTH:(patterns + f + 1) * DEPTH, :])
            x = x if f == 2 else 0.5 * x
            for c, y in enumerate(spread(x)):
                US[f, c, base:base + DEPTH, :] = y

    enter(q_lo, f_lo, DEPTH, None)
    enter(q_hi, f_hi, DEPTH + rows - DEPTH, None)

    to_right.wait()
    to_left.wait()

    @pl.when(has_down)
    def _():
        strip_down.start()

    @pl.when(has_up)
    def _():
        strip_up.start()

    def masked_half(half, x):
        return jnp.where(half_ok, x, 0.0) if half else x

    def strip(side, half, pick):
        if half:
            x = jnp.where(lane < cols // 2, pick(bot_ref, side), pick(top_ref, side))
            return masked_half(1, x)
        return pick(mid_ref, side)

    scale = jnp.where(sub < 2, 0.5, 1.0)

    def enter_strip(half):
        for side in range(2):
            x = scale * strip(side, half, lambda ref, sd: ref[sd, members + patterns:members + patterns + 8, :])
            for c, y in enumerate(spread(x)):
                UH[side, c, half] = y
            for c, y in enumerate(forced(strip(side, half, lambda ref, sd: ref[sd, members:members + patterns, :]))):
                FH[side, c, half] = y
            ys = butterfly([strip(side, half, lambda ref, sd: ref[sd, pl.ds(v, 8, stride=8), :]) for v in range(8)])
            for c in range(8):
                H[0, side, c, half] = ys[c]

    enter_strip(0)

    @pl.when(has_down)
    def _():
        for c in ups:
            c.wait_recv()
        strip_up_recv = rdma(mid_ref, bot_ref, gy_send.at[1], gy_recv.at[1], {"gy": up})
        strip_up_recv.wait_recv()

    @pl.when(has_up)
    def _():
        for c in downs:
            c.wait_recv()
        strip_down.wait_recv()

    enter(qt_ref, ft_ref, 0, has_up)
    enter(qb_ref, fb_ref, DEPTH + rows, has_down)
    enter_strip(1)

    def masked(i, x):
        if i < DEPTH:
            return jnp.where(has_up, x, 0.0)
        if i >= DEPTH + rows:
            return jnp.where(has_down, x, 0.0)
        return x

    first, last = lane < 8, lane >= cols - 8

    def place(i):
        j = i - DEPTH
        return (0, j) if 0 <= j < rows else (1, (i - DEPTH - rows) % n_rows)

    def across(x, get, i):
        half, j = place(i)
        left = jnp.where(first, roll(get(0, 7, half), -8 * j), roll(x(7), 8))
        right = jnp.where(last, roll(get(1, 0, half), cols - 8 - 8 * j), roll(x(0), -8))
        return left, right

    def inward(x, lo, hi):
        left = [jnp.zeros(shape, F32)] * 2
        right = [jnp.zeros(shape, F32)] * 2
        for i in range(lo, hi):
            half, j = place(i)
            here = block0 == 8 * j
            left[half] = jnp.where(here, roll(x(i, 0), 8 * j), left[half])
            right[half] = jnp.where(here, roll(x(i, 7), 8 * j - (cols - 8)), right[half])
        return left, right

    def vertical(m, t):
        mn, tn, mp, tp = roll(m, -8), roll(t, -8), roll(m, 8), roll(t, 8)
        return ((jnp.where(last, tn, mn), jnp.where(last, mn, tn)),
                (jnp.where(first, tp, mp), jnp.where(first, mp, tp)))

    zero = jnp.zeros(shape, F32)

    def halo_x(get, ins, side, c, half):
        left, right = ins
        if c > 0:
            xm = get(side, c - 1, half)
        else:
            xm = right[half] if side == 1 else zero
        if c < 7:
            xp = get(side, c + 1, half)
        else:
            xp = left[half] if side == 0 else zero
        return xm, xp

    for s in range(STEPS):
        src, dst = s % 2, (s + 1) % 2
        lo, hi = 2 * s, n_rows - 2 * s
        final = s == STEPS - 1
        qa = lambda i, c: Q[src, i, c]
        qh = lambda side, c, half: H[src, side, c, half]
        lh = lambda side, c, half: LH[side, c, half]
        la = lambda i, c: L[i, c]
        ins = inward(qa, lo, hi)
        grads = {}
        for side in range(2):
            for c in range(8):
                m, t = qh(side, c, 0), qh(side, c, 1)
                nxt, prv = vertical(m, t)
                for half in range(2):
                    mid = (m, t)[half]
                    xm, xp = halo_x(qh, ins, side, c, half)
                    lap = (nxt[half] + prv[half]) + (xp + xm) - 4.0 * mid
                    LH[side, c, half] = masked_half(half, lap)
                    if not final:
                        grads[side, c, half] = (UH[side, c, half, 0:1] * (xp - xm)
                                                + UH[side, c, half, 1:2] * (nxt[half] - prv[half]))
        adv = {}
        def first_pass(i):
            left, right = across(lambda c: qa(i, c), qh, i)
            row = [qa(i, c) for c in range(8)]
            for c in range(8):
                xm = row[c - 1] if c else left
                xp = row[c + 1] if c < 7 else right
                up_, dn = qa(i + 1, c), qa(i - 1, c)
                L[i, c] = masked(i, (up_ + dn) + (xp + xm) - 4.0 * row[c])
                if lo + 2 <= i < hi - 2:
                    adv[i, c] = (US[0, c, i:i + 1, :] * (xp - xm) + US[1, c, i:i + 1, :] * (up_ - dn))
                    adv[i, c] = keep * row[c] + (FO[i, c] - adv[i, c])

        def second_pass(i):
            left, right = across(lambda c: la(i, c), lh, i)
            row = [la(i, c) for c in range(8)]
            outs = []
            for c in range(8):
                xm = row[c - 1] if c else left
                xp = row[c + 1] if c < 7 else right
                bi = (la(i + 1, c) + la(i - 1, c)) + (xp + xm) - 4.0 * row[c]
                new = (adv.pop((i, c)) + (diffuse * row[c] - hyper * bi)) * US[2, c, i:i + 1, :]
                if final:
                    outs.append(new)
                else:
                    Q[dst, i, c] = new
            if final:
                for v, y in enumerate(butterfly(outs)):
                    out_ref[pl.ds(v * rows + i - DEPTH, 8, stride=8 * rows), :] = y

        first_pass(lo + 1)
        first_pass(lo + 2)
        for i in range(lo + 2, hi - 2):
            first_pass(i + 1)
            second_pass(i)
        if final:
            break
        ins = inward(la, lo + 1, hi - 1)
        for side in range(2):
            for c in range(8):
                m, t = lh(side, c, 0), lh(side, c, 1)
                nxt, prv = vertical(m, t)
                for half in range(2):
                    mid = (m, t)[half]
                    xm, xp = halo_x(lh, ins, side, c, half)
                    bi = (nxt[half] + prv[half]) + (xp + xm) - 4.0 * mid
                    new = (keep * qh(side, c, half) + (FH[side, c, half] - grads[side, c, half])
                           + (diffuse * mid - hyper * bi))
                    H[dst, side, c, half] = new * UH[side, c, half, 2:3]

    index = index_ref[0]
    col = jnp.bitwise_and(index, cols - 1)
    row = jnp.right_shift(index, cols.bit_length() - 1)
    hot = (lax.broadcasted_iota(I32, (cols, cols), 0) == col).astype(jnp.bfloat16)
    row_id = lax.broadcasted_iota(I32, (8, rows, cols), 1)
    dot = functools.partial(jnp.dot, preferred_element_type=F32)
    for g in range(members // 8):
        x = out_ref[pl.ds(g * 8 * rows, 8 * rows), :]
        x1 = x.astype(jnp.bfloat16)
        rem = x - x1.astype(F32)
        x2 = rem.astype(jnp.bfloat16)
        x3 = (rem - x2.astype(F32)).astype(jnp.bfloat16)
        picked = dot(x1, hot) + (dot(x2, hot) + dot(x3, hot))
        obs_ref[pl.ds(g * 8, 8), :] = jnp.sum(
            jnp.where(row_id == row[None], picked.reshape(8, rows, cols), 0.0), axis=1)

    mine = pl.ds(pl.multiple_of(ens * members, members), members)
    obs_copies, th_copies = [], []
    for k, p in enumerate(others):
        obs_copies.append(rdma(obs_ref, obs_all.at[mine], ens_send.at[2 * k], ens_recv.at[2 * k], {"ens": p}))
        th_copies.append(rdma(theta_ref, th_ref.at[ens], ens_send.at[2 * k + 1], ens_recv.at[2 * k + 1], {"ens": p}))
    for c in obs_copies + th_copies:
        c.start()
    store = pltpu.make_async_copy(out_ref, final_ref, store_sem.at[0])
    store.start()
    obs_all[mine, :] = obs_ref[...]
    th_ref[ens] = theta_ref[...]
    for c in obs_copies:
        c.wait()

    x = obs_all[...]
    mean = jnp.mean(x, axis=0, keepdims=True)
    inv = 1.0 / sig_ref[0]
    anom = (x - mean) * inv
    d = jnp.broadcast_to((val_ref[0] - mean) * inv, (8, x.shape[1]))
    nt = (((1,), (1,)), ((), ()))
    total = x.shape[0]
    c_part = lax.dot_general(d, anom, nt, preferred_element_type=F32, precision=HIGH)[0:1]
    gram = lax.dot_general(anom, anom, nt, preferred_element_type=F32, precision=HIGH)

    def finish():
        to_send = [(has_down, downs + [strip_down]), (has_up, ups + [strip_up])]
        for ok, copies in to_send:
            @pl.when(ok)
            def _():
                for c in copies:
                    c.wait_send()
        for c in th_copies:
            c.wait()
        store.wait()

    if not reduce_here:
        full_ref[...] = gram
        c_ref[...] = c_part
        finish()
        return
    c_own[...] = c_part
    part[...] = gram
    own = total // n
    at = lambda p: pl.ds(pl.multiple_of(p * own, own), own)
    sends = [rdma(part.at[at(p)], rs.at[k], rs_send.at[k], rs_recv.at[k], w)
             for k, (p, w) in enumerate(zip(peers, where))]
    c_sends = [rdma(c_own, cs.at[k], cs_send.at[k], cs_recv.at[k], w) for k, w in enumerate(where)]
    for c in sends + c_sends:
        c.start()
    acc = part[at(me), :]
    for k, c in enumerate(sends):
        c.wait_recv()
        acc = acc + rs[k]
    full_ref[at(me), :] = acc
    gathers = [rdma(full_ref.at[at(me)], full_ref.at[at(me)], ag_send.at[k], ag_recv.at[k], w)
               for k, w in enumerate(where)]
    for c in gathers:
        c.start()
    acc = c_own[...]
    for k, c in enumerate(c_sends):
        c.wait_recv()
        acc = acc + cs[k]
    c_ref[...] = acc
    for c in sends + c_sends:
        c.wait_send()
    finish()
    for c in gathers:
        c.wait()


def run_step(mesh, state, forcing, u_vel, v_vel, land, member_mode, theta, obs_index, values, sigma):
    n_gx, n_gy, n_ens = mesh.shape["gx"], mesh.shape["gy"], mesh.shape["ens"]
    members, rows, cols = state.shape
    patterns = forcing.shape[0]
    sites = obs_index.shape[-1]
    params = theta.shape[1]
    nf = -(-(patterns + 3) // 8) * 8
    strips = members + nf
    n_rows = rows + 2 * DEPTH
    total = members * n_ens
    n = n_gx * n_gy
    reduce_here = total % (8 * n) == 0
    own = total // n if reduce_here else 8
    slots = n - 1 if reduce_here else 1
    sds = jax.ShapeDtypeStruct
    dma = pltpu.SemaphoreType.DMA
    reg = (8, cols)
    final, full, c, th = pl.pallas_call(
        functools.partial(step_kernel, n_gx, n_gy, n_ens, reduce_here),
        out_shape=[sds((members * rows, cols), F32), sds((total, total), F32), sds((1, total), F32),
                   sds((n_ens, params, members), F32)],
        in_specs=[anyspec()] * 10,
        out_specs=[anyspec()] + [vspec()] * 3,
        scratch_shapes=[VM((members, DEPTH, cols), F32)] * 2 + [VM((nf, DEPTH, cols), F32)] * 2
        + [VM((rows, cols), I32), VM((1, members), I32), VM((params, members), F32), VM((1, 1, sites), I32),
           VM((1, 1, sites), F32), VM((1, 1, sites), F32)]
        + [VM((members, DEPTH, cols), F32)] * 2 + [VM((nf, DEPTH, cols), F32)] * 2
        + [VM((2, strips, cols), F32)] * 4
        + [VM((2, n_rows, 8) + reg, F32), VM((n_rows, 8) + reg, F32), VM((n_rows, 8) + reg, F32),
           VM((3, 8, n_rows, cols), F32),
           VM((2, 2, 8, 2) + reg, F32), VM((2, 8, 2) + reg, F32), VM((2, 8, 2) + reg, F32),
           VM((2, 8, 2) + reg, F32), VM(reg, F32), VM((members * rows, cols), F32)]
        + [VM((members, sites), F32), VM((total, sites), F32), VM((total, total), F32), VM((slots, own, total), F32),
           VM((1, total), F32), VM((slots, 1, total), F32)]
        + [dma((14,)), dma((1,)), dma((4,)), dma((4,)), dma((2,)), dma((2,)), dma((2,)), dma((2,))]
        + [dma((2 * (n_ens - 1),))] * 2 + [dma((slots,))] * 6,
        compiler_params=pltpu.CompilerParams(collective_id=0, has_side_effects=True),
        name="step",
    )(state, forcing, u_vel, v_vel, land, member_mode.reshape(1, members), theta.T, obs_index, values, sigma)
    if not reduce_here:
        full, c = lax.psum((full, c), ("gx", "gy"))
    return final, full, c, th


def solve_kernel(members, full_ref, c_ref, th_ref, out_ref, xs):
    total = full_ref.shape[0]
    blocks = total // 8
    n_ens, params = th_ref.shape[0], th_ref.shape[1]
    shape = (8, total)
    lane = lax.broadcasted_iota(jnp.int32, shape, 1)
    sub = lax.broadcasted_iota(jnp.int32, shape, 0)
    tht = jnp.concatenate([th_ref[e] for e in range(n_ens)], axis=1)
    spread = tht - jnp.mean(tht, axis=1, keepdims=True)
    xs[...] = jnp.zeros_like(xs)
    xs[0:params, :] = spread
    cols_of = xs[...].T
    A, R = [], []
    for k in range(blocks):
        rows = slice(8 * k, 8 * k + 8)
        A.append(full_ref[rows, :] + jnp.where(lane == sub + 8 * k, float(total - 1), 0.0))
        R.append(cols_of[rows])

    def splat(x):
        return jnp.broadcast_to(x, shape)

    for k in range(blocks):
        rs_, rr = [], []
        d = {}
        for j in range(8):
            row = splat(A[k][j:j + 1])
            rs_.append(row)
            rr.append(splat(R[k][j:j + 1]))
            for i in range(j, 8):
                d[j, i] = splat(row[:, 8 * k + i:8 * k + i + 1])
        inv = []
        for j in range(8):
            inv.append(1.0 / d[j, j])
            for i in range(j + 1, 8):
                m = d[j, i] * inv[j]
                rs_[i] = rs_[i] - m * rs_[j]
                rr[i] = rr[i] - m * rr[j]
                for q in range(i, 8):
                    d[i, q] = d[i, q] - m * d[j, q]
        for i in reversed(range(8)):
            for j in range(i + 1, 8):
                rs_[i] = rs_[i] - d[i, j] * rs_[j]
                rr[i] = rr[i] - d[i, j] * rr[j]
            rs_[i] = rs_[i] * inv[i]
            rr[i] = rr[i] * inv[i]
        a, r = rs_[7], rr[7]
        for j in range(7):
            a = jnp.where(sub == j, rs_[j], a)
            r = jnp.where(sub == j, rr[j], r)
        A[k], R[k] = a, r
        for i in list(range(k + 1, blocks)) + list(range(k)):
            a, r = A[i], R[i]
            for j in range(8):
                c = splat(A[i][:, 8 * k + j:8 * k + j + 1])
                if k + 1 < blocks:
                    a = a - c * rs_[j]
                r = r - c * rr[j]
            A[i], R[i] = a, r
    for k in range(blocks):
        xs[8 * k:8 * k + 8, :] = R[k]
    x = xs[...].T[0:8]
    shift = jnp.sum(x * c_ref[...], axis=1, keepdims=True)
    new = (jnp.mean(tht, axis=1, keepdims=True) + shift[0:params]) + float(total - 1) * x[0:params]
    ens = lax.axis_index("ens")
    for e in range(n_ens):
        @pl.when(ens == e)
        def _():
            out_ref[...] = new[:, e * members:(e + 1) * members]


def relay_kernel(members, full_ref, c_ref, th_ref, raw_ref, out_ref, final_ref, xs, buf, sem):
    take = pltpu.make_async_copy(raw_ref, buf, sem.at[0])
    take.start()
    take.wait()
    give = pltpu.make_async_copy(buf, final_ref, sem.at[1])
    give.start()
    solve_kernel(members, full_ref, c_ref, th_ref, out_ref, xs)
    give.wait()


def solve(full, c, th, theta, raw):
    out, final = pl.pallas_call(
        functools.partial(relay_kernel, theta.shape[0]),
        out_shape=[jax.ShapeDtypeStruct(theta.shape[::-1], F32), jax.ShapeDtypeStruct(raw.shape, F32)],
        in_specs=[vspec()] * 3 + [anyspec()],
        out_specs=[vspec(), anyspec()],
        scratch_shapes=[VM(full.shape, F32), VM(raw.shape, F32), pltpu.SemaphoreType.DMA((2,))],
        name="solve",
    )(full, c, th, raw)
    return out.T, final


def local(mesh, state, u_vel, v_vel, land, forcing, member_mode, theta, obs_index, obs_values, obs_sigma):
    raw, full, c, th = run_step(mesh, state, forcing, u_vel, v_vel, land, member_mode, theta, obs_index,
                                obs_values, obs_sigma)
    new_theta, final = solve(full, c, th, theta, raw)
    return final.reshape(state.shape), new_theta


def solution(mesh):
    placed = (
        P("ens", "gy", "gx"),
        P("gy", "gx"),
        P("gy", "gx"),
        P("gy", "gx"),
        P(None, "gy", "gx"),
        P("ens"),
        P("ens", None),
        P("gy", "gx", None),
        P("gy", "gx", None),
        P("gy", "gx", None),
    )
    return jax.shard_map(
        functools.partial(local, mesh),
        mesh=mesh,
        in_specs=placed,
        out_specs=(P("ens", "gy", "gx"), P("ens", None)),
        check_vma=False,
    )
```

```python
import functools
import jax
import jax.numpy as jnp
from jax import lax
from jax.experimental import pallas as pl
from jax.experimental.pallas import tpu as pltpu
from jax.sharding import PartitionSpec as P

STEPS = 4
SPACE = 24 * 2**20
SMALL_SPACE = 12 * 2**20
DEPTH = 2 * STEPS
F32 = jnp.float32
I32 = jnp.int32
VM = pltpu.VMEM
MESH = pl.DeviceIdType.MESH
HIGH = lax.Precision.HIGHEST


def vspec():
    return pl.BlockSpec(memory_space=pltpu.VMEM)


def anyspec():
    return pl.BlockSpec(memory_space=pl.ANY)


def hspec():
    return pl.BlockSpec(memory_space=pltpu.HBM)


def flat(ref):
    return ref.reshape(ref.shape[0] * ref.shape[1], ref.shape[2])


def rdma(src, dst, send, recv, dev):
    return pltpu.make_async_remote_copy(src_ref=src, dst_ref=dst, send_sem=send, recv_sem=recv,
                                        device_id=dev, device_id_type=MESH)


def step_kernel(n_gx, n_gy, n_ens, reduce_here, owners,
                state_ref, forcing_ref, u_ref, v_ref, land_ref, mode_in, theta_in, index_in, val_in, sig_in,
                out_lo, out_hi, full_ref, th_ref,
                q_lo, q_hi, f_lo, f_hi, land_b, mode_ref, theta_ref, index_ref, val_ref, sig_ref,
                qt_ref, qb_ref, ft_ref, fb_ref, pack, corner, mid_ref, top_ref, bot_ref,
                Q, L, FO, US, H, LH, FH, UH, TH,
                obs_ref, obs_all, part, rs,
                load_sem, row_send, row_recv, gx_send, gx_recv, diag_send, diag_recv,
                ens_send, ens_recv, rs_send, rs_recv, ag_send, ag_recv):
    gx, gy, ens = lax.axis_index("gx"), lax.axis_index("gy"), lax.axis_index("ens")
    right, left = lax.rem(gx + 1, n_gx), lax.rem(gx + n_gx - 1, n_gx)
    has_up, has_down = gy > 0, gy < n_gy - 1
    up, down = jnp.maximum(gy - 1, 0), jnp.minimum(gy + 1, n_gy - 1)
    members, rows, cols = state_ref.shape
    patterns = forcing_ref.shape[0]
    fields = patterns + 3
    n_rows = rows + 2 * DEPTH
    n = n_gx * n_gy
    me = gy * n_gx + gx
    peers = [lax.rem(me + o, n) for o in range(1, n)] if reduce_here else []
    where = [{"gx": lax.rem(p, n_gx), "gy": lax.div(p, n_gx)} for p in peers]
    others = [lax.rem(ens + o, n_ens) for o in range(1, n_ens)]

    pairs = [(state_ref.at[:, 0:DEPTH, :], q_lo), (state_ref.at[:, rows - DEPTH:, :], q_hi)]
    for h, dst in ((0, f_lo), (rows - DEPTH, f_hi)):
        pairs += [(forcing_ref.at[:, h:h + DEPTH, :], dst.at[0:patterns]),
                  (u_ref.at[h:h + DEPTH, :], dst.at[patterns]), (v_ref.at[h:h + DEPTH, :], dst.at[patterns + 1])]
    pairs += [(land_ref, land_b), (mode_in, mode_ref), (theta_in, theta_ref), (index_in, index_ref),
              (val_in, val_ref), (sig_in, sig_ref)]
    loads = [pltpu.make_async_copy(s, d, load_sem.at[k]) for k, (s, d) in enumerate(pairs)]
    for c in loads:
        c.start()

    barrier = pltpu.get_barrier_semaphore()

    def greet(dev):
        pl.semaphore_signal(barrier, inc=1, device_id=dev, device_id_type=MESH)

    if reduce_here:
        for d in where:
            greet(d)
        expected = len(where)
    else:
        sides = 2
        expected = sides
        for dev in (right, left):
            greet({"gx": dev})
        for ok, dev in ((has_up, up), (has_down, down)):
            @pl.when(ok)
            def _():
                greet({"gy": dev})
                for other in (right, left):
                    greet({"gx": other, "gy": dev})
            expected = expected + (1 + sides) * ok.astype(I32)
    for p in others:
        greet({"ens": p})
    expected = expected + len(others)

    shape = (8, cols)
    lane = lax.broadcasted_iota(I32, shape, 1)
    sub = lax.broadcasted_iota(I32, shape, 0)
    low = jnp.bitwise_and(lane, 7)
    block0 = lane - low
    block = jnp.right_shift(lane, 3)
    blocks = cols // 8
    bits = [jnp.bitwise_and(lane, k) != 0 for k in (1, 2, 4)]
    first, last = lane < 8, lane >= cols - 8

    def roll(x, k):
        return pltpu.roll(x, k % cols, 1) if k % cols else x

    def gather(x, idx, axis):
        return jnp.take_along_axis(x, idx, axis=axis, mode="promise_in_bounds")

    def skew(xs):
        return [roll(x, v) for v, x in enumerate(xs)]

    def unskew(ys):
        for k, bit in zip((1, 2, 4), bits):
            ys = [jnp.where(bit, ys[(u + k) & 7], ys[u]) for u in range(8)]
        return [roll(ys[-c & 7], -c) for c in range(8)]

    slot = [0]
    queue = {}

    def at_slot(t, fn):
        if t <= slot[0]:
            fn()
        else:
            queue.setdefault(t, []).append(fn)

    def tick():
        slot[0] += 1
        for fn in queue.pop(slot[0], []):
            fn()

    def drain():
        while queue:
            tick()

    LAT = 3

    for c in loads:
        c.wait()
    for h, dst in ((0, f_lo), (rows - DEPTH, f_hi)):
        dst[patterns + 2] = (1 - land_b[h:h + DEPTH, :]).astype(F32)
        dst[fields:] = jnp.zeros((dst.shape[0] - fields, DEPTH, cols), F32)

    pl.semaphore_wait(barrier, expected)

    downs = [rdma(q_hi, qt_ref, row_send.at[0], row_recv.at[0], {"gy": down}),
             rdma(f_hi.at[0:fields], ft_ref.at[0:fields], row_send.at[1], row_recv.at[1], {"gy": down})]
    ups = [rdma(q_lo, qb_ref, row_send.at[2], row_recv.at[2], {"gy": up}),
           rdma(f_lo.at[0:fields], fb_ref.at[0:fields], row_send.at[3], row_recv.at[3], {"gy": up})]
    dests = (right, left)
    fall = [rdma(corner.at[sd, 0], top_ref.at[sd], diag_send.at[sd], diag_recv.at[sd], {"gx": dests[sd], "gy": down})
            for sd in range(2)]
    rise = [rdma(corner.at[sd, 1], bot_ref.at[sd], diag_send.at[2 + sd], diag_recv.at[2 + sd],
                 {"gx": dests[sd], "gy": up}) for sd in range(2)]

    @pl.when(has_down)
    def _():
        for c in downs:
            c.start()

    @pl.when(has_up)
    def _():
        for c in ups:
            c.start()

    half_blocks = blocks // 2
    row_at = [2 * ((b - DEPTH // 2) % half_blocks) + (1 if (b - DEPTH // 2) % blocks >= half_blocks else 0)
              for b in range(blocks)]
    left_half = lane < cols // 2

    def pack_from(lo_ref, hi_ref, base):
        for g in range(lo_ref.shape[0] // 8):
            vals = []
            for r in range(rows):
                ref = flat(lo_ref if r < DEPTH else hi_ref)
                vals.append(ref[pl.ds(g * 8 * DEPTH + r % DEPTH, 8, stride=DEPTH), :])
            moved = [roll(jnp.where(left_half, vals[row_at[(b + 2) % blocks]], vals[row_at[b]]), 8 * b + 8)
                     for b in range(blocks)]
            hi, lo = moved[0], moved[0]
            for b in range(1, blocks):
                hi = jnp.where(block == b, moved[b], hi)
                lo = jnp.where(block == (b + 1) % blocks, moved[b], lo)
            packed.append((hi, lo))
            for sd in range(2):
                pack[sd, base + g * 8:base + g * 8 + 8, :] = packed[-1][sd]

    packed = []
    logical = [jnp.bitwise_and(block + sd, blocks - 1) for sd in range(2)]
    low_half = [jnp.bitwise_and(x, DEPTH // 2) == 0 for x in logical]
    pack_from(q_lo, q_hi, 0)
    pack_from(f_lo, f_hi, members)
    to_right = rdma(pack.at[0], mid_ref.at[0], gx_send.at[0], gx_recv.at[0], {"gx": right})
    to_left = rdma(pack.at[1], mid_ref.at[1], gx_send.at[1], gx_recv.at[1], {"gx": left})
    to_right.start()
    to_left.start()
    for p in range(len(packed) // 2):
        for sd in range(2):
            x, y = packed[2 * p][sd], roll(packed[2 * p + 1][sd], cols // 4)
            corner[sd, 0, p * 8:p * 8 + 8, :] = jnp.where(low_half[sd], x, y)
            corner[sd, 1, p * 8:p * 8 + 8, :] = jnp.where(low_half[sd], y, x)

    @pl.when(has_down)
    def _():
        for c in fall:
            c.start()

    @pl.when(has_up)
    def _():
        for c in rise:
            c.start()

    TH[...] = jnp.zeros_like(TH)
    TH[0:theta_ref.shape[0], 0:members] = theta_ref[...]
    member = low * 8 + sub
    par = [gather(jnp.broadcast_to(TH[k:k + 1, :], shape), member, 1) for k in range(4)]
    diffuse = 0.05 * (1.0 + 0.5 * jnp.tanh(par[0]))
    hyper = 0.005 * (1.0 + 0.5 * jnp.tanh(par[1]))
    keep = 1.0 - 0.05 * (1.0 + 0.5 * jnp.tanh(par[2]))
    gain = par[3]
    mrow = jnp.concatenate([mode_ref[...], jnp.zeros((1, cols - members), I32)], axis=1)
    pattern_of = gather(jnp.broadcast_to(mrow, shape), member, 1)

    def spread(x):
        return [gather(x, block0 + c, 1) for c in range(8)]

    def place(i):
        return i & 1, (i >> 1) % blocks

    def edge_acc():
        return {"l": [jnp.zeros(shape, F32)] * 2, "r": [jnp.zeros(shape, F32)] * 2}

    def inward(acc, i, x0, x7):
        half, j = place(i)
        g = roll(jnp.where(last, x7, x0), 8 * j)

        def put():
            acc["l"][half] = jnp.where(block == j, g, acc["l"][half])
            acc["r"][half] = jnp.where(block == (j - 1) % blocks, g, acc["r"][half])
        at_slot(slot[0] + LAT, put)

    acc_q = edge_acc()

    def enter(ref, fr, base, ok):
        ref, fr = flat(ref), flat(fr)

        def keep_in(x):
            return x if ok is None else jnp.where(ok, x, 0.0)

        def start(k):
            ys = skew([keep_in(ref[pl.ds(v * 8 * DEPTH + k, 8, stride=DEPTH), :]) for v in range(8)])
            zs = spread(keep_in(fr[pl.ds(k, 8, stride=DEPTH), :]))

            def middle():
                os = unskew(ys)
                for c in range(8):
                    FO[base + k, c] = gain * gather(zs[c], pattern_of, 0)

                def end():
                    for c in range(8):
                        Q[0, base + k, c] = os[c]
                    inward(acc_q, base + k, os[0], os[7])
                at_slot(slot[0] + LAT, end)
            at_slot(slot[0] + LAT, middle)

        for k in range(DEPTH):
            start(k)
            tick()
        for f in range(3):
            x = keep_in(fr[(patterns + f) * DEPTH:(patterns + f + 1) * DEPTH, :])
            x = x if f == 2 else 0.5 * x
            zs = spread(x)

            def keep_us(f=f, zs=zs):
                for c, y in enumerate(zs):
                    US[f, c, base:base + DEPTH, :] = y
            at_slot(slot[0] + LAT, keep_us)
            tick()

    enter(q_lo, f_lo, DEPTH, None)
    enter(q_hi, f_hi, DEPTH + rows - DEPTH, None)
    drain()

    @pl.when(has_down)
    def _():
        for c in ups:
            c.wait_recv()

    @pl.when(has_up)
    def _():
        for c in downs:
            c.wait_recv()

    enter(qt_ref, ft_ref, 0, has_up)
    enter(qb_ref, fb_ref, DEPTH + rows, has_down)
    drain()

    to_right.wait_recv()
    to_left.wait_recv()

    @pl.when(has_down)
    def _():
        for c in rise:
            c.wait_recv()

    @pl.when(has_up)
    def _():
        for c in fall:
            c.wait_recv()

    edge_ok, inner = [], []
    quarter = DEPTH // 2
    for side in range(2):
        ok = jnp.where(logical[side] < quarter, has_up.astype(I32),
                       jnp.where(logical[side] >= blocks - quarter, has_down.astype(I32), 1))
        edge_ok.append(ok > 0)
        inner.append((logical[side] >= quarter) & (logical[side] < blocks - quarter))

    def strip(side, g):
        p = g // 2
        mid = mid_ref[side, g * 8:g * 8 + 8, :]
        top, bot = top_ref[side, p * 8:p * 8 + 8, :], bot_ref[side, p * 8:p * 8 + 8, :]
        if g % 2:
            ends = roll(jnp.where(low_half[side], bot, top), -(cols // 4))
        else:
            ends = jnp.where(low_half[side], top, bot)
        even = jnp.where(inner[side], mid, roll(ends, cols // 2))
        odd = jnp.where(inner[side], roll(mid, cols // 2), ends)
        return [jnp.where(edge_ok[side], x, 0.0) for x in (even, odd)]

    scale = jnp.where(sub < 2, 0.5, 1.0)
    for side in range(2):
        both = [strip(side, v) for v in range(8)]
        cells = strip(side, members // 8)
        extra = strip(side, members // 8 + 1)
        for half in range(2):
            def start(side=side, half=half, both=both, cells=cells, extra=extra):
                ys = skew([b[half] for b in both])
                zs = spread(cells[half])
                ws = spread(scale * extra[half])

                def middle():
                    os = unskew(ys)
                    for c in range(8):
                        FH[side, c, half] = gain * gather(zs[c], pattern_of, 0)
                        UH[side, c, half] = ws[c]

                    def end():
                        for c in range(8):
                            H[0, side, c, half] = os[c]
                    at_slot(slot[0] + LAT, end)
                at_slot(slot[0] + LAT, middle)
            at_slot(slot[0] + 2, start)
            tick()
    drain()

    def masked(i, x):
        if i < DEPTH:
            return jnp.where(has_up, x, 0.0)
        if i >= DEPTH + rows:
            return jnp.where(has_down, x, 0.0)
        return x

    def across(x0, x7, get, i):
        half, j = place(i)
        f = roll(jnp.where(block == j, get(0, 7, half), get(1, 0, half)), -8 * j)
        return jnp.where(first, f, roll(x7, 8)), jnp.where(last, f, roll(x0, -8))

    def vertical(get, side, c):
        m, t = get(side, c, 0), get(side, c, 1)
        return (t, roll(t, 8)), (roll(m, -8), m)

    def halo_x(get, acc, side, c, half):
        if c > 0:
            xm = get(side, c - 1, half)
        else:
            xm = acc["r"][half] if side == 1 else jnp.zeros(shape, F32)
        if c < 7:
            xp = get(side, c + 1, half)
        else:
            xp = acc["l"][half] if side == 0 else jnp.zeros(shape, F32)
        return xm, xp

    def live(side, least):
        return range(least, 8) if side == 0 else range(0, 8 - least)

    def advance(s, acc_in):
        src, dst = s % 2, (s + 1) % 2
        lo, hi = 2 * s, n_rows - 2 * s
        final = s == STEPS - 1
        acc_l, acc_out = edge_acc(), edge_acc()
        qh = lambda side, c, half: H[src, side, c, half]
        lh = lambda side, c, half: LH[side, c, half]
        grads, adv, turn1, turn2, hv, lv = {}, {}, {}, {}, {}, {}
        lap_cells = [(0, 7), (1, 0)] if final else [(sd, c) for sd in range(2) for c in live(sd, lo + 1)]
        new_cells = [] if final else [(sd, c) for sd in range(2) for c in live(sd, lo + 2)]

        def halo_rolls():
            for sd, c in lap_cells:
                hv[sd, c] = vertical(qh, sd, c)

        def halo_lap():
            for sd, c in lap_cells:
                for half in range(2):
                    nxt, prv = hv[sd, c][half]
                    xm, xp = halo_x(qh, acc_in, sd, c, half)
                    lap = (nxt + prv) + (xp + xm) - 4.0 * qh(sd, c, half)
                    LH[sd, c, half] = jnp.where(edge_ok[sd], lap, 0.0)
                    if (sd, c) in new_cells:
                        grads[sd, c, half] = (UH[sd, c, half, 0:1] * (xp - xm) + UH[sd, c, half, 1:2] * (nxt - prv))

        def lap_rolls():
            for sd, c in new_cells:
                lv[sd, c] = vertical(lh, sd, c)

        def halo_new():
            for sd, c in new_cells:
                for half in range(2):
                    nxt, prv = lv[sd, c][half]
                    xm, xp = halo_x(lh, acc_l, sd, c, half)
                    mid = lh(sd, c, half)
                    bi = (nxt + prv) + (xp + xm) - 4.0 * mid
                    new = (keep * qh(sd, c, half) + (FH[sd, c, half] - grads[sd, c, half])
                           + (diffuse * mid - hyper * bi))
                    H[dst, sd, c, half] = new * UH[sd, c, half, 2:3]

        def turn_first(i):
            turn1[i] = across(Q[src, i, 0], Q[src, i, 7], qh, i)

        def first_pass(i):
            left, right = turn1.pop(i)
            row = [Q[src, i, c] for c in range(8)]
            laps = []
            for c in range(8):
                xm = row[c - 1] if c else left
                xp = row[c + 1] if c < 7 else right
                up_, dn = Q[src, i + 1, c], Q[src, i - 1, c]
                laps.append(masked(i, (up_ + dn) + (xp + xm) - 4.0 * row[c]))
                L[i, c] = laps[c]
                if lo + 2 <= i < hi - 2:
                    a = US[0, c, i:i + 1, :] * (xp - xm) + US[1, c, i:i + 1, :] * (up_ - dn)
                    adv[i, c] = keep * row[c] + (FO[i, c] - a)
            if not final:
                inward(acc_l, i, laps[0], laps[7])
            if lo + 2 <= i < hi - 2:
                turn2[i] = across(laps[0], laps[7], lh, i)

        def second_pass(i):
            left, right = turn2.pop(i)
            row = [L[i, c] for c in range(8)]
            outs = []
            for c in range(8):
                xm = row[c - 1] if c else left
                xp = row[c + 1] if c < 7 else right
                bi = (L[i + 1, c] + L[i - 1, c]) + (xp + xm) - 4.0 * row[c]
                new = (adv.pop((i, c)) + (diffuse * row[c] - hyper * bi)) * US[2, c, i:i + 1, :]
                outs.append(new)
                if not final:
                    Q[dst, i, c] = new
            if not final:
                inward(acc_out, i, outs[0], outs[7])
                return
            ys = skew(outs)

            def middle():
                xs = unskew(ys)

                def end():
                    r = i - DEPTH
                    ref = flat(out_lo if r < DEPTH else out_hi)
                    for v, x in enumerate(xs):
                        ref[pl.ds(v * 8 * DEPTH + r % DEPTH, 8, stride=DEPTH), :] = x
                at_slot(slot[0] + LAT, end)
            at_slot(slot[0] + LAT, middle)

        halo_rolls()
        for k in range(LAT):
            turn_first(lo + 1 + k)
        while any(fn.__name__ == "put" for fns in queue.values() for fn in fns):
            tick()
        halo_lap()
        lap_rolls()
        for i in range(lo + 1, hi - 1):
            if i + LAT < hi - 1:
                turn_first(i + LAT)
            first_pass(i)
            if lo + 2 <= i < hi - 2:
                at_slot(slot[0] + LAT, functools.partial(second_pass, i))
            tick()
        for _ in range(LAT):
            tick()
        if not final:
            halo_new()
        return acc_out

    acc = acc_q
    for s in range(STEPS):
        acc = advance(s, acc)
    drain()

    index = index_ref[0]
    col = jnp.bitwise_and(index, cols - 1)
    row = jnp.right_shift(index, cols.bit_length() - 1)
    hot = (lax.broadcasted_iota(I32, (cols, cols), 0) == col).astype(jnp.bfloat16)
    row_id = lax.broadcasted_iota(I32, (8, DEPTH, cols), 1)
    dot = functools.partial(jnp.dot, preferred_element_type=F32)
    for g in range(members // 8):
        found = []
        for h, ref in ((0, out_lo), (rows - DEPTH, out_hi)):
            x = flat(ref)[pl.ds(g * 8 * DEPTH, 8 * DEPTH), :]
            x1 = x.astype(jnp.bfloat16)
            rem = x - x1.astype(F32)
            x2 = rem.astype(jnp.bfloat16)
            x3 = (rem - x2.astype(F32)).astype(jnp.bfloat16)
            picked = dot(x1, hot) + (dot(x2, hot) + dot(x3, hot))
            found.append(jnp.where(row_id + h == row[None], picked.reshape(8, DEPTH, cols), 0.0))
        obs_ref[pl.ds(g * 8, 8), :] = jnp.sum(found[0] + found[1], axis=1)

    mine = pl.ds(pl.multiple_of(ens * members, members), members)
    obs_copies, th_copies = [], []
    for k, p in enumerate(others):
        obs_copies.append(rdma(obs_ref, obs_all.at[mine], ens_send.at[2 * k], ens_recv.at[2 * k], {"ens": p}))
        th_copies.append(rdma(theta_ref, th_ref.at[ens], ens_send.at[2 * k + 1], ens_recv.at[2 * k + 1], {"ens": p}))
    for c in obs_copies + th_copies:
        c.start()
    obs_all[mine, :] = obs_ref[...]
    th_ref[ens] = theta_ref[...]
    for c in obs_copies:
        c.wait()

    x = obs_all[...]
    mean = jnp.mean(x, axis=0, keepdims=True)
    inv = 1.0 / sig_ref[0]
    anom = (x - mean) * inv
    d = jnp.broadcast_to((val_ref[0] - mean) * inv, (8, x.shape[1]))
    total = x.shape[0]
    gram = lax.dot_general(jnp.concatenate([anom, d], axis=0), anom, (((1,), (1,)), ((), ())),
                           preferred_element_type=F32, precision=HIGH)

    def finish():
        for c in (to_right, to_left):
            c.wait_send()
        for ok, copies in ((has_down, fall + downs), (has_up, rise + ups)):
            @pl.when(ok)
            def _():
                for c in copies:
                    c.wait_send()
        for c in th_copies:
            c.wait()

    if not reduce_here:
        full_ref[...] = gram
        finish()
        return
    part[...] = gram
    own = total // len(owners)
    spans = [pl.ds(k * own, own + (8 if k == len(owners) - 1 else 0)) for k in range(len(owners))]
    rank = [oy * n_gx + ox for ox, oy in owners]

    def to_owner(k, slot_):
        return rdma(part.at[spans[k]], rs.at[slot_, 0:spans[k].size], rs_send.at[k], rs_recv.at[slot_],
                    {"gx": owners[k][0], "gy": owners[k][1]})

    def from_owner(k, j):
        return rdma(full_ref.at[spans[k]], full_ref.at[spans[k]], ag_send.at[j], ag_recv.at[k], where[j])

    for k in range(len(owners)):
        @pl.when(me != rank[k])
        def _():
            to_owner(k, me).start()
    for k in range(len(owners)):
        @pl.when(me == rank[k])
        def _():
            acc = part[spans[k], :]
            for p in range(n):
                if p != rank[k]:
                    to_owner(k, p).wait_recv()
                    acc = acc + rs[p, 0:spans[k].size, :]
            full_ref[spans[k], :] = acc
            for j in range(len(where)):
                from_owner(k, j).start()
    for k in range(len(owners)):
        @pl.when(me != rank[k])
        def _():
            to_owner(k, me).wait_send()
    finish()
    for k in range(len(owners)):
        @pl.when(me != rank[k])
        def _():
            from_owner(k, 0).wait_recv()

        @pl.when(me == rank[k])
        def _():
            for j in range(len(where)):
                from_owner(k, j).wait_send()


def run_step(mesh, state, forcing, u_vel, v_vel, land, member_mode, theta, obs_index, values, sigma):
    n_gx, n_gy, n_ens = mesh.shape["gx"], mesh.shape["gy"], mesh.shape["ens"]
    members, rows, cols = state.shape
    patterns = forcing.shape[0]
    sites = obs_index.shape[-1]
    params = theta.shape[1]
    nf = -(-(patterns + 3) // 8) * 8
    strips = members + nf
    n_rows = rows + 2 * DEPTH
    total = members * n_ens
    n = n_gx * n_gy
    owners = [(ox, oy) for oy in range(1, n_gy, 2) for ox in sorted({max(n_gx // 2 - 1, 0), n_gx // 2})]
    reduce_here = 0 < n <= 32 and len(owners) > 0 and total % (8 * len(owners)) == 0
    own = total // len(owners) + 8 if reduce_here else 8
    slots = n if reduce_here else 1
    sds = jax.ShapeDtypeStruct
    dma = pltpu.SemaphoreType.DMA
    reg = (8, cols)
    out_lo, out_hi, full, th = pl.pallas_call(
        functools.partial(step_kernel, n_gx, n_gy, n_ens, reduce_here, owners),
        out_shape=[sds((members, DEPTH, cols), F32)] * 2 + [sds((total + 8, total), F32),
                   sds((n_ens, params, members), F32)],
        in_specs=[hspec()] * 10,
        out_specs=[vspec()] * 4,
        scratch_shapes=[VM((members, DEPTH, cols), F32)] * 2 + [VM((nf, DEPTH, cols), F32)] * 2
        + [VM((rows, cols), I32), VM((1, members), I32), VM((params, members), F32), VM((1, 1, sites), I32),
           VM((1, 1, sites), F32), VM((1, 1, sites), F32)]
        + [VM((members, DEPTH, cols), F32)] * 2 + [VM((nf, DEPTH, cols), F32)] * 2
        + [VM((2, strips, cols), F32), VM((2, 2, strips // 2, cols), F32), VM((2, strips, cols), F32)]
        + [VM((2, strips // 2, cols), F32)] * 2
        + [VM((2, n_rows, 8) + reg, F32), VM((n_rows, 8) + reg, F32), VM((n_rows, 8) + reg, F32),
           VM((3, 8, n_rows, cols), F32),
           VM((2, 2, 8, 2) + reg, F32), VM((2, 8, 2) + reg, F32), VM((2, 8, 2) + reg, F32),
           VM((2, 8, 2) + reg, F32), VM(reg, F32)]
        + [VM((members, sites), F32), VM((total, sites), F32), VM((total + 8, total), F32), VM((slots, own, total), F32)]
        + [dma((14,)), dma((4,)), dma((4,)), dma((2,)), dma((2,)), dma((4,)), dma((4,))]
        + [dma((2 * (n_ens - 1),))] * 2 + [dma((slots,))] * 4,
        compiler_params=pltpu.CompilerParams(collective_id=0, has_side_effects=True, vmem_limit_bytes=SPACE),
        name="step",
    )(*[pltpu.with_memory_space_constraint(x, pltpu.HBM) for x in
        (state, forcing, u_vel, v_vel, land, member_mode.reshape(1, members), theta.T, obs_index, values, sigma)])
    if not reduce_here:
        full = lax.psum(full, ("gx", "gy"))
    return out_lo, out_hi, full, th


def solve_kernel(members, full_ref, th_ref, out_ref, xs):
    total = full_ref.shape[1]
    blocks = total // 8
    n_ens, params = th_ref.shape[0], th_ref.shape[1]
    shape = (8, total)
    lane = lax.broadcasted_iota(jnp.int32, shape, 1)
    sub = lax.broadcasted_iota(jnp.int32, shape, 0)
    tht = jnp.concatenate([th_ref[e] for e in range(n_ens)], axis=1)
    spread = tht - jnp.mean(tht, axis=1, keepdims=True)
    xs[...] = jnp.zeros_like(xs)
    xs[0:params, :] = spread
    cols_of = xs[...].T
    A, R = [], []
    for k in range(blocks):
        rows = slice(8 * k, 8 * k + 8)
        A.append(full_ref[rows, :] + jnp.where(lane == sub + 8 * k, float(total - 1), 0.0))
        R.append(cols_of[rows])

    def splat(x):
        return jnp.broadcast_to(x, shape)

    for k in range(blocks):
        rs_, rr = [], []
        d = {}
        for j in range(8):
            row = splat(A[k][j:j + 1])
            rs_.append(row)
            rr.append(splat(R[k][j:j + 1]))
            for i in range(j, 8):
                d[j, i] = splat(row[:, 8 * k + i:8 * k + i + 1])
        inv = []
        for j in range(8):
            inv.append(1.0 / d[j, j])
            for i in range(j + 1, 8):
                m = d[j, i] * inv[j]
                rs_[i] = rs_[i] - m * rs_[j]
                rr[i] = rr[i] - m * rr[j]
                for q in range(i, 8):
                    d[i, q] = d[i, q] - m * d[j, q]
        for i in reversed(range(8)):
            for j in range(i + 1, 8):
                rs_[i] = rs_[i] - d[i, j] * rs_[j]
                rr[i] = rr[i] - d[i, j] * rr[j]
            rs_[i] = rs_[i] * inv[i]
            rr[i] = rr[i] * inv[i]
        a, r = rs_[7], rr[7]
        for j in range(7):
            a = jnp.where(sub == j, rs_[j], a)
            r = jnp.where(sub == j, rr[j], r)
        A[k], R[k] = a, r
        for i in list(range(k + 1, blocks)) + list(range(k)):
            a, r = A[i], R[i]
            for j in range(8):
                c = splat(A[i][:, 8 * k + j:8 * k + j + 1])
                if k + 1 < blocks:
                    a = a - c * rs_[j]
                r = r - c * rr[j]
            A[i], R[i] = a, r
    for k in range(blocks):
        xs[8 * k:8 * k + 8, :] = R[k]
    x = xs[...].T[0:8]
    shift = jnp.sum(x * full_ref[total:total + 1, :], axis=1, keepdims=True)
    new = (jnp.mean(tht, axis=1, keepdims=True) + shift[0:params]) + float(total - 1) * x[0:params]
    ens = lax.axis_index("ens")
    for e in range(n_ens):
        @pl.when(ens == e)
        def _():
            out_ref[...] = new[:, e * members:(e + 1) * members]


def relay_kernel(members, full_ref, th_ref, lo_ref, hi_ref, out_ref, final_ref, xs, sem):
    depth, rows = lo_ref.shape[1], final_ref.shape[1]
    gives = [pltpu.make_async_copy(lo_ref, final_ref.at[:, 0:depth, :], sem.at[0]),
             pltpu.make_async_copy(hi_ref, final_ref.at[:, rows - depth:, :], sem.at[1])]
    for c in gives:
        c.start()
    solve_kernel(members, full_ref, th_ref, out_ref, xs)
    for c in gives:
        c.wait()


def solve(full, th, theta, lo, hi, shape):
    total = full.shape[1]
    out, final = pl.pallas_call(
        functools.partial(relay_kernel, theta.shape[0]),
        out_shape=[jax.ShapeDtypeStruct(theta.shape[::-1], F32), jax.ShapeDtypeStruct(shape, F32)],
        in_specs=[vspec()] * 4,
        out_specs=[vspec(), hspec()],
        scratch_shapes=[VM((total, total), F32), pltpu.SemaphoreType.DMA((2,))],
        compiler_params=pltpu.CompilerParams(vmem_limit_bytes=SMALL_SPACE),
        name="solve",
    )(full, th, lo, hi)
    return out.T, final


def local(mesh, state, u_vel, v_vel, land, forcing, member_mode, theta, obs_index, obs_values, obs_sigma):
    lo, hi, full, th = run_step(mesh, state, forcing, u_vel, v_vel, land, member_mode, theta, obs_index,
                                obs_values, obs_sigma)
    new_theta, final = solve(full, th, theta, lo, hi, state.shape)
    return final, new_theta


def solution(mesh):
    placed = (
        P("ens", "gy", "gx"),
        P("gy", "gx"),
        P("gy", "gx"),
        P("gy", "gx"),
        P(None, "gy", "gx"),
        P("ens"),
        P("ens", None),
        P("gy", "gx", None),
        P("gy", "gx", None),
        P("gy", "gx", None),
    )
    return jax.shard_map(
        functools.partial(local, mesh),
        mesh=mesh,
        in_specs=placed,
        out_specs=(P("ens", "gy", "gx"), P("ens", None)),
        check_vma=False,
    )
```

```python
import functools
import jax
import jax.numpy as jnp
from jax import lax
from jax.experimental import pallas as pl
from jax.experimental.pallas import tpu as pltpu
from jax.sharding import PartitionSpec as P

STEPS = 4
SPACE = 24 * 2**20
SMALL_SPACE = 12 * 2**20
DEPTH = 2 * STEPS
F32 = jnp.float32
I32 = jnp.int32
VM = pltpu.VMEM
MESH = pl.DeviceIdType.MESH
HIGH = lax.Precision.HIGHEST


def vspec():
    return pl.BlockSpec(memory_space=pltpu.VMEM)


def anyspec():
    return pl.BlockSpec(memory_space=pl.ANY)


def hspec():
    return pl.BlockSpec(memory_space=pltpu.HBM)


def flat(ref):
    return ref.reshape(ref.shape[0] * ref.shape[1], ref.shape[2])


def rdma(src, dst, send, recv, dev):
    return pltpu.make_async_remote_copy(src_ref=src, dst_ref=dst, send_sem=send, recv_sem=recv,
                                        device_id=dev, device_id_type=MESH)


def step_kernel(n_gx, n_gy, n_ens, reduce_here, owners,
                state_ref, forcing_ref, u_ref, v_ref, land_ref, mode_in, theta_in, index_in, val_in, sig_in,
                out_lo, out_hi, full_ref, th_ref,
                q_lo, q_hi, f_lo, f_hi, land_b, mode_ref, theta_ref, index_ref, val_ref, sig_ref,
                qt_ref, qb_ref, ft_ref, fb_ref, pack, corner, mid_ref, top_ref, bot_ref,
                Q, L, FO, US, H, LH, FH, UH, TH,
                obs_ref, obs_all, part, rs,
                load_sem, row_send, row_recv, gx_send, gx_recv, diag_send, diag_recv,
                ens_send, ens_recv, rs_send, rs_recv, ag_send, ag_recv):
    gx, gy, ens = lax.axis_index("gx"), lax.axis_index("gy"), lax.axis_index("ens")
    right, left = lax.rem(gx + 1, n_gx), lax.rem(gx + n_gx - 1, n_gx)
    has_up, has_down = gy > 0, gy < n_gy - 1
    up, down = jnp.maximum(gy - 1, 0), jnp.minimum(gy + 1, n_gy - 1)
    members, rows, cols = state_ref.shape
    patterns = forcing_ref.shape[0]
    fields = patterns + 3
    n_rows = rows + 2 * DEPTH
    n = n_gx * n_gy
    me = gy * n_gx + gx
    peers = [lax.rem(me + o, n) for o in range(1, n)] if reduce_here else []
    where = [{"gx": lax.rem(p, n_gx), "gy": lax.div(p, n_gx)} for p in peers]
    others = [lax.rem(ens + o, n_ens) for o in range(1, n_ens)]

    pairs = [(state_ref.at[:, 0:DEPTH, :], q_lo), (state_ref.at[:, rows - DEPTH:, :], q_hi)]
    for h, dst in ((0, f_lo), (rows - DEPTH, f_hi)):
        pairs += [(forcing_ref.at[:, h:h + DEPTH, :], dst.at[0:patterns]),
                  (u_ref.at[h:h + DEPTH, :], dst.at[patterns]), (v_ref.at[h:h + DEPTH, :], dst.at[patterns + 1])]
    pairs += [(land_ref, land_b), (mode_in, mode_ref), (theta_in, theta_ref), (index_in, index_ref),
              (val_in, val_ref), (sig_in, sig_ref)]
    loads = [pltpu.make_async_copy(s, d, load_sem.at[k]) for k, (s, d) in enumerate(pairs)]
    for c in loads:
        c.start()

    barrier = pltpu.get_barrier_semaphore()

    def greet(dev):
        pl.semaphore_signal(barrier, inc=1, device_id=dev, device_id_type=MESH)

    if reduce_here:
        for d in where:
            greet(d)
        expected = len(where)
    else:
        sides = 2
        expected = sides
        for dev in (right, left):
            greet({"gx": dev})
        for ok, dev in ((has_up, up), (has_down, down)):
            @pl.when(ok)
            def _():
                greet({"gy": dev})
                for other in (right, left):
                    greet({"gx": other, "gy": dev})
            expected = expected + (1 + sides) * ok.astype(I32)
    for p in others:
        greet({"ens": p})
    expected = expected + len(others)

    shape = (8, cols)
    lane = lax.broadcasted_iota(I32, shape, 1)
    sub = lax.broadcasted_iota(I32, shape, 0)
    low = jnp.bitwise_and(lane, 7)
    block0 = lane - low
    block = jnp.right_shift(lane, 3)
    blocks = cols // 8
    bits = [jnp.bitwise_and(lane, k) != 0 for k in (1, 2, 4)]
    first, last = lane < 8, lane >= cols - 8

    def roll(x, k):
        return pltpu.roll(x, k % cols, 1) if k % cols else x

    def gather(x, idx, axis):
        return jnp.take_along_axis(x, idx, axis=axis, mode="promise_in_bounds")

    def skew(xs):
        return [roll(x, v) for v, x in enumerate(xs)]

    def unskew(ys):
        for k, bit in zip((1, 2, 4), bits):
            ys = [jnp.where(bit, ys[(u + k) & 7], ys[u]) for u in range(8)]
        return [roll(ys[-c & 7], -c) for c in range(8)]

    slot = [0]
    queue = {}

    def at_slot(t, fn):
        if t <= slot[0]:
            fn()
        else:
            queue.setdefault(t, []).append(fn)

    def tick():
        slot[0] += 1
        for fn in queue.pop(slot[0], []):
            fn()

    def drain():
        while queue:
            tick()

    LAT = 3

    for c in loads:
        c.wait()
    for h, dst in ((0, f_lo), (rows - DEPTH, f_hi)):
        dst[patterns + 2] = (1 - land_b[h:h + DEPTH, :]).astype(F32)
        dst[fields:] = jnp.zeros((dst.shape[0] - fields, DEPTH, cols), F32)

    pl.semaphore_wait(barrier, expected)

    half_rows = DEPTH // 2
    near = [slice(0, half_rows), slice(half_rows, DEPTH)]
    downs = [rdma(f_hi.at[0:fields], ft_ref.at[0:fields], row_send.at[0], row_recv.at[0], {"gy": down})]
    ups = [rdma(f_lo.at[0:fields], fb_ref.at[0:fields], row_send.at[3], row_recv.at[3], {"gy": up})]
    for k, r in enumerate(near):
        downs.append(rdma(q_hi.at[:, r, :], qt_ref.at[:, r, :], row_send.at[1 + k], row_recv.at[1 + k], {"gy": down}))
        ups.append(rdma(q_lo.at[:, r, :], qb_ref.at[:, r, :], row_send.at[4 + k], row_recv.at[4 + k], {"gy": up}))
    dests = (right, left)
    fall = [rdma(corner.at[sd, 0], top_ref.at[sd], diag_send.at[sd], diag_recv.at[sd], {"gx": dests[sd], "gy": down})
            for sd in range(2)]
    rise = [rdma(corner.at[sd, 1], bot_ref.at[sd], diag_send.at[2 + sd], diag_recv.at[2 + sd],
                 {"gx": dests[sd], "gy": up}) for sd in range(2)]

    @pl.when(has_down)
    def _():
        for c in downs:
            c.start()

    @pl.when(has_up)
    def _():
        for c in ups:
            c.start()

    half_blocks = blocks // 2
    row_at = [2 * ((b - DEPTH // 2) % half_blocks) + (1 if (b - DEPTH // 2) % blocks >= half_blocks else 0)
              for b in range(blocks)]
    left_half = lane < cols // 2

    def pack_from(lo_ref, hi_ref, base):
        for g in range(lo_ref.shape[0] // 8):
            vals = []
            for r in range(rows):
                ref = flat(lo_ref if r < DEPTH else hi_ref)
                vals.append(ref[pl.ds(g * 8 * DEPTH + r % DEPTH, 8, stride=DEPTH), :])
            moved = [roll(jnp.where(left_half, vals[row_at[(b + 2) % blocks]], vals[row_at[b]]), 8 * b + 8)
                     for b in range(blocks)]
            hi, lo = moved[0], moved[0]
            for b in range(1, blocks):
                hi = jnp.where(block == b, moved[b], hi)
                lo = jnp.where(block == (b + 1) % blocks, moved[b], lo)
            packed.append((hi, lo))
            for sd in range(2):
                pack[sd, base + g * 8:base + g * 8 + 8, :] = packed[-1][sd]

    packed = []
    logical = [jnp.bitwise_and(block + sd, blocks - 1) for sd in range(2)]
    low_half = [jnp.bitwise_and(x, DEPTH // 2) == 0 for x in logical]
    pack_from(q_lo, q_hi, 0)
    pack_from(f_lo, f_hi, members)
    to_right = rdma(pack.at[0], mid_ref.at[0], gx_send.at[0], gx_recv.at[0], {"gx": right})
    to_left = rdma(pack.at[1], mid_ref.at[1], gx_send.at[1], gx_recv.at[1], {"gx": left})
    to_right.start()
    to_left.start()
    for p in range(len(packed) // 2):
        for sd in range(2):
            x, y = packed[2 * p][sd], roll(packed[2 * p + 1][sd], cols // 4)
            corner[sd, 0, p * 8:p * 8 + 8, :] = jnp.where(low_half[sd], x, y)
            corner[sd, 1, p * 8:p * 8 + 8, :] = jnp.where(low_half[sd], y, x)

    @pl.when(has_down)
    def _():
        for c in fall:
            c.start()

    @pl.when(has_up)
    def _():
        for c in rise:
            c.start()

    TH[...] = jnp.zeros_like(TH)
    TH[0:theta_ref.shape[0], 0:members] = theta_ref[...]
    member = low * 8 + sub
    par = [gather(jnp.broadcast_to(TH[k:k + 1, :], shape), member, 1) for k in range(4)]
    diffuse = 0.05 * (1.0 + 0.5 * jnp.tanh(par[0]))
    hyper = 0.005 * (1.0 + 0.5 * jnp.tanh(par[1]))
    lap_gain = diffuse + 4.0 * hyper
    keep = 1.0 - 0.05 * (1.0 + 0.5 * jnp.tanh(par[2]))
    gain = par[3]
    mrow = jnp.concatenate([mode_ref[...], jnp.zeros((1, cols - members), I32)], axis=1)
    pattern_of = gather(jnp.broadcast_to(mrow, shape), member, 1)

    def spread(x):
        return [gather(x, block0 + c, 1) for c in range(8)]

    def place(i):
        return i & 1, (i >> 1) % blocks

    def edge_acc():
        return {"l": [jnp.zeros(shape, F32)] * 2, "r": [jnp.zeros(shape, F32)] * 2}

    def inward(acc, i, x0, x7):
        half, j = place(i)
        g = roll(jnp.where(last, x7, x0), 8 * j)

        def put():
            acc["l"][half] = jnp.where(block == j, g, acc["l"][half])
            acc["r"][half] = jnp.where(block == (j - 1) % blocks, g, acc["r"][half])
        at_slot(slot[0] + LAT, put)

    acc_q = edge_acc()

    def kept(ok, x):
        return x if ok is None else jnp.where(ok, x, 0.0)

    def enter_row(ref, k, base, ok):
        ref = flat(ref)
        ys = skew([kept(ok, ref[pl.ds(v * 8 * DEPTH + k, 8, stride=DEPTH), :]) for v in range(8)])

        def middle():
            os = unskew(ys)

            def end():
                for c in range(8):
                    Q[0, base + k, c] = os[c]
                inward(acc_q, base + k, os[0], os[7])
            at_slot(slot[0] + LAT, end)
        at_slot(slot[0] + LAT, middle)

    def enter_field_row(fr, k, base, ok):
        zs = spread(kept(ok, flat(fr)[pl.ds(k, 8, stride=DEPTH), :]))

        def end():
            for c in range(8):
                FO[base + k, c] = gain * gather(zs[c], pattern_of, 0)
        at_slot(slot[0] + LAT, end)

    def enter_planes(fr, base, ok):
        for f in range(3):
            x = kept(ok, flat(fr)[(patterns + f) * DEPTH:(patterns + f + 1) * DEPTH, :])
            x = x if f == 2 else 0.5 * x
            zs = spread(x)

            def end(f=f, zs=zs):
                for c, y in enumerate(zs):
                    US[f, c, base:base + DEPTH, :] = y
            at_slot(slot[0] + LAT, end)
            tick()

    def await_rows(k):
        @pl.when(has_down)
        def _():
            ups[k].wait_recv()

        @pl.when(has_up)
        def _():
            downs[k].wait_recv()

    for ref, fr, base in ((q_lo, f_lo, DEPTH), (q_hi, f_hi, rows)):
        for k in range(DEPTH):
            enter_row(ref, k, base, None)
            enter_field_row(fr, k, base, None)
            tick()
        enter_planes(fr, base, None)
    drain()

    await_rows(0)
    for fr, base, ok in ((ft_ref, 0, has_up), (fb_ref, DEPTH + rows, has_down)):
        for k in range(DEPTH):
            enter_field_row(fr, k, base, ok)
            tick()
        enter_planes(fr, base, ok)
    drain()
    for part_ in range(len(near)):
        await_rows(1 + part_)
        for ref, base, ok in ((qt_ref, 0, has_up), (qb_ref, DEPTH + rows, has_down)):
            for k in range(near[part_].start, near[part_].stop):
                enter_row(ref, k, base, ok)
                tick()
        drain()

    to_right.wait_recv()
    to_left.wait_recv()

    @pl.when(has_down)
    def _():
        for c in rise:
            c.wait_recv()

    @pl.when(has_up)
    def _():
        for c in fall:
            c.wait_recv()

    edge_ok, inner = [], []
    quarter = DEPTH // 2
    for side in range(2):
        ok = jnp.where(logical[side] < quarter, has_up.astype(I32),
                       jnp.where(logical[side] >= blocks - quarter, has_down.astype(I32), 1))
        edge_ok.append(ok > 0)
        inner.append((logical[side] >= quarter) & (logical[side] < blocks - quarter))

    def strip(side, g):
        p = g // 2
        mid = mid_ref[side, g * 8:g * 8 + 8, :]
        top, bot = top_ref[side, p * 8:p * 8 + 8, :], bot_ref[side, p * 8:p * 8 + 8, :]
        if g % 2:
            ends = roll(jnp.where(low_half[side], bot, top), -(cols // 4))
        else:
            ends = jnp.where(low_half[side], top, bot)
        even = jnp.where(inner[side], mid, roll(ends, cols // 2))
        odd = jnp.where(inner[side], roll(mid, cols // 2), ends)
        return [jnp.where(edge_ok[side], x, 0.0) for x in (even, odd)]

    scale = jnp.where(sub < 2, 0.5, 1.0)
    for side in range(2):
        both = [strip(side, v) for v in range(8)]
        cells = strip(side, members // 8)
        extra = strip(side, members // 8 + 1)
        for half in range(2):
            def start(side=side, half=half, both=both, cells=cells, extra=extra):
                ys = skew([b[half] for b in both])
                zs = spread(cells[half])
                ws = spread(scale * extra[half])

                def middle():
                    os = unskew(ys)
                    for c in range(8):
                        FH[side, c, half] = gain * gather(zs[c], pattern_of, 0)
                        UH[side, c, half] = ws[c]

                    def end():
                        for c in range(8):
                            H[0, side, c, half] = os[c]
                    at_slot(slot[0] + LAT, end)
                at_slot(slot[0] + LAT, middle)
            at_slot(slot[0] + 2, start)
            tick()
    drain()

    def masked(i, x):
        if i < DEPTH:
            return jnp.where(has_up, x, 0.0)
        if i >= DEPTH + rows:
            return jnp.where(has_down, x, 0.0)
        return x

    def across(x0, x7, get, i):
        half, j = place(i)
        f = roll(jnp.where(block == j, get(0, 7, half), get(1, 0, half)), -8 * j)
        return jnp.where(first, f, roll(x7, 8)), jnp.where(last, f, roll(x0, -8))

    def vertical(get, side, c):
        m, t = get(side, c, 0), get(side, c, 1)
        return (t, roll(t, 8)), (roll(m, -8), m)

    def halo_x(get, acc, side, c, half):
        if c > 0:
            xm = get(side, c - 1, half)
        else:
            xm = acc["r"][half] if side == 1 else jnp.zeros(shape, F32)
        if c < 7:
            xp = get(side, c + 1, half)
        else:
            xp = acc["l"][half] if side == 0 else jnp.zeros(shape, F32)
        return xm, xp

    def live(side, least):
        return range(least, 8) if side == 0 else range(0, 8 - least)

    def advance(s, acc_in):
        src, dst = s % 2, (s + 1) % 2
        lo, hi = 2 * s, n_rows - 2 * s
        final = s == STEPS - 1
        acc_l, acc_out = edge_acc(), edge_acc()
        qh = lambda side, c, half: H[src, side, c, half]
        lh = lambda side, c, half: LH[side, c, half]
        grads, adv, turn1, turn2, hv, lv = {}, {}, {}, {}, {}, {}
        lap_cells = [(0, 7), (1, 0)] if final else [(sd, c) for sd in range(2) for c in live(sd, lo + 1)]
        new_cells = [] if final else [(sd, c) for sd in range(2) for c in live(sd, lo + 2)]

        def halo_rolls():
            for sd, c in lap_cells:
                hv[sd, c] = vertical(qh, sd, c)

        def halo_lap():
            for sd, c in lap_cells:
                for half in range(2):
                    nxt, prv = hv[sd, c][half]
                    xm, xp = halo_x(qh, acc_in, sd, c, half)
                    lap = (nxt + prv) + (xp + xm) - 4.0 * qh(sd, c, half)
                    LH[sd, c, half] = jnp.where(edge_ok[sd], lap, 0.0)
                    if (sd, c) in new_cells:
                        grads[sd, c, half] = (UH[sd, c, half, 0:1] * (xp - xm) + UH[sd, c, half, 1:2] * (nxt - prv))

        def lap_rolls():
            for sd, c in new_cells:
                lv[sd, c] = vertical(lh, sd, c)

        def halo_new():
            for sd, c in new_cells:
                for half in range(2):
                    nxt, prv = lv[sd, c][half]
                    xm, xp = halo_x(lh, acc_l, sd, c, half)
                    mid = lh(sd, c, half)
                    around = (nxt + prv) + (xp + xm)
                    new = (keep * qh(sd, c, half) + (FH[sd, c, half] - grads[sd, c, half])
                           + (lap_gain * mid - hyper * around))
                    H[dst, sd, c, half] = new * UH[sd, c, half, 2:3]

        def turn_first(i):
            turn1[i] = across(Q[src, i, 0], Q[src, i, 7], qh, i)

        def first_pass(i):
            left, right = turn1.pop(i)
            row = [Q[src, i, c] for c in range(8)]
            laps = []
            for c in range(8):
                xm = row[c - 1] if c else left
                xp = row[c + 1] if c < 7 else right
                up_, dn = Q[src, i + 1, c], Q[src, i - 1, c]
                laps.append(masked(i, (up_ + dn) + (xp + xm) - 4.0 * row[c]))
                L[i, c] = laps[c]
                if lo + 2 <= i < hi - 2:
                    a = US[0, c, i:i + 1, :] * (xp - xm) + US[1, c, i:i + 1, :] * (up_ - dn)
                    adv[i, c] = keep * row[c] + (FO[i, c] - a)
            if not final:
                inward(acc_l, i, laps[0], laps[7])
            if lo + 2 <= i < hi - 2:
                turn2[i] = across(laps[0], laps[7], lh, i)

        def second_pass(i):
            left, right = turn2.pop(i)
            row = [L[i, c] for c in range(8)]
            outs = []
            for c in range(8):
                xm = row[c - 1] if c else left
                xp = row[c + 1] if c < 7 else right
                around = (L[i + 1, c] + L[i - 1, c]) + (xp + xm)
                new = (adv.pop((i, c)) + (lap_gain * row[c] - hyper * around)) * US[2, c, i:i + 1, :]
                outs.append(new)
                if not final:
                    Q[dst, i, c] = new
            if not final:
                inward(acc_out, i, outs[0], outs[7])
                return
            ys = skew(outs)

            def middle():
                xs = unskew(ys)

                def end():
                    r = i - DEPTH
                    ref = flat(out_lo if r < DEPTH else out_hi)
                    for v, x in enumerate(xs):
                        ref[pl.ds(v * 8 * DEPTH + r % DEPTH, 8, stride=DEPTH), :] = x
                at_slot(slot[0] + LAT, end)
            at_slot(slot[0] + LAT, middle)

        halo_rolls()
        for k in range(LAT):
            turn_first(lo + 1 + k)
        while any(fn.__name__ == "put" for fns in queue.values() for fn in fns):
            tick()
        halo_lap()
        lap_rolls()
        for i in range(lo + 1, hi - 1):
            if i + LAT < hi - 1:
                turn_first(i + LAT)
            first_pass(i)
            if lo + 2 <= i < hi - 2:
                at_slot(slot[0] + LAT, functools.partial(second_pass, i))
            tick()
        for _ in range(LAT):
            tick()
        if not final:
            halo_new()
        return acc_out

    acc = acc_q
    for s in range(STEPS):
        acc = advance(s, acc)
    drain()

    index = index_ref[0]
    col = jnp.bitwise_and(index, cols - 1)
    row = jnp.right_shift(index, cols.bit_length() - 1)
    hot = (lax.broadcasted_iota(I32, (cols, cols), 0) == col).astype(jnp.bfloat16)
    row_id = lax.broadcasted_iota(I32, (8, DEPTH, cols), 1)
    dot = functools.partial(jnp.dot, preferred_element_type=F32)
    for g in range(members // 8):
        found = []
        for h, ref in ((0, out_lo), (rows - DEPTH, out_hi)):
            x = flat(ref)[pl.ds(g * 8 * DEPTH, 8 * DEPTH), :]
            x1 = x.astype(jnp.bfloat16)
            rem = x - x1.astype(F32)
            x2 = rem.astype(jnp.bfloat16)
            x3 = (rem - x2.astype(F32)).astype(jnp.bfloat16)
            picked = dot(x1, hot) + (dot(x2, hot) + dot(x3, hot))
            found.append(jnp.where(row_id + h == row[None], picked.reshape(8, DEPTH, cols), 0.0))
        obs_ref[pl.ds(g * 8, 8), :] = jnp.sum(found[0] + found[1], axis=1)

    mine = pl.ds(pl.multiple_of(ens * members, members), members)
    obs_copies, th_copies = [], []
    for k, p in enumerate(others):
        obs_copies.append(rdma(obs_ref, obs_all.at[mine], ens_send.at[2 * k], ens_recv.at[2 * k], {"ens": p}))
        th_copies.append(rdma(theta_ref, th_ref.at[ens], ens_send.at[2 * k + 1], ens_recv.at[2 * k + 1], {"ens": p}))
    for c in obs_copies + th_copies:
        c.start()
    obs_all[mine, :] = obs_ref[...]
    th_ref[ens] = theta_ref[...]
    for c in obs_copies:
        c.wait()

    x = obs_all[...]
    mean = jnp.mean(x, axis=0, keepdims=True)
    inv = 1.0 / sig_ref[0]
    anom = (x - mean) * inv
    d = jnp.broadcast_to((val_ref[0] - mean) * inv, (8, x.shape[1]))
    total = x.shape[0]
    gram = lax.dot_general(jnp.concatenate([anom, d], axis=0), anom, (((1,), (1,)), ((), ())),
                           preferred_element_type=F32, precision=HIGH)

    def finish():
        for c in (to_right, to_left):
            c.wait_send()
        for ok, copies in ((has_down, fall + downs), (has_up, rise + ups)):
            @pl.when(ok)
            def _():
                for c in copies:
                    c.wait_send()
        for c in th_copies:
            c.wait()

    if not reduce_here:
        full_ref[...] = gram
        finish()
        return
    part[...] = gram
    own = total // len(owners)
    spans = [pl.ds(k * own, own + (8 if k == len(owners) - 1 else 0)) for k in range(len(owners))]
    rank = [oy * n_gx + ox for ox, oy in owners]

    def to_owner(k, slot_):
        return rdma(part.at[spans[k]], rs.at[slot_, 0:spans[k].size], rs_send.at[k], rs_recv.at[slot_],
                    {"gx": owners[k][0], "gy": owners[k][1]})

    def from_owner(k, j):
        return rdma(full_ref.at[spans[k]], full_ref.at[spans[k]], ag_send.at[j], ag_recv.at[k], where[j])

    for k in range(len(owners)):
        @pl.when(me != rank[k])
        def _():
            to_owner(k, me).start()
    for k in range(len(owners)):
        @pl.when(me == rank[k])
        def _():
            acc = part[spans[k], :]
            for p in range(n):
                if p != rank[k]:
                    to_owner(k, p).wait_recv()
                    acc = acc + rs[p, 0:spans[k].size, :]
            full_ref[spans[k], :] = acc
            for j in range(len(where)):
                from_owner(k, j).start()
    for k in range(len(owners)):
        @pl.when(me != rank[k])
        def _():
            to_owner(k, me).wait_send()
    finish()
    for k in range(len(owners)):
        @pl.when(me != rank[k])
        def _():
            from_owner(k, 0).wait_recv()

        @pl.when(me == rank[k])
        def _():
            for j in range(len(where)):
                from_owner(k, j).wait_send()


def run_step(mesh, state, forcing, u_vel, v_vel, land, member_mode, theta, obs_index, values, sigma):
    n_gx, n_gy, n_ens = mesh.shape["gx"], mesh.shape["gy"], mesh.shape["ens"]
    members, rows, cols = state.shape
    patterns = forcing.shape[0]
    sites = obs_index.shape[-1]
    params = theta.shape[1]
    nf = -(-(patterns + 3) // 8) * 8
    strips = members + nf
    n_rows = rows + 2 * DEPTH
    total = members * n_ens
    n = n_gx * n_gy
    owners = [(ox, oy) for oy in range(1, n_gy, 2) for ox in sorted({max(n_gx // 2 - 1, 0), n_gx // 2})]
    reduce_here = 0 < n <= 32 and len(owners) > 0 and total % (8 * len(owners)) == 0
    own = total // len(owners) + 8 if reduce_here else 8
    slots = n if reduce_here else 1
    sds = jax.ShapeDtypeStruct
    dma = pltpu.SemaphoreType.DMA
    reg = (8, cols)
    out_lo, out_hi, full, th = pl.pallas_call(
        functools.partial(step_kernel, n_gx, n_gy, n_ens, reduce_here, owners),
        out_shape=[sds((members, DEPTH, cols), F32)] * 2 + [sds((total + 8, total), F32),
                   sds((n_ens, params, members), F32)],
        in_specs=[hspec()] * 10,
        out_specs=[vspec()] * 4,
        scratch_shapes=[VM((members, DEPTH, cols), F32)] * 2 + [VM((nf, DEPTH, cols), F32)] * 2
        + [VM((rows, cols), I32), VM((1, members), I32), VM((params, members), F32), VM((1, 1, sites), I32),
           VM((1, 1, sites), F32), VM((1, 1, sites), F32)]
        + [VM((members, DEPTH, cols), F32)] * 2 + [VM((nf, DEPTH, cols), F32)] * 2
        + [VM((2, strips, cols), F32), VM((2, 2, strips // 2, cols), F32), VM((2, strips, cols), F32)]
        + [VM((2, strips // 2, cols), F32)] * 2
        + [VM((2, n_rows, 8) + reg, F32), VM((n_rows, 8) + reg, F32), VM((n_rows, 8) + reg, F32),
           VM((3, 8, n_rows, cols), F32),
           VM((2, 2, 8, 2) + reg, F32), VM((2, 8, 2) + reg, F32), VM((2, 8, 2) + reg, F32),
           VM((2, 8, 2) + reg, F32), VM(reg, F32)]
        + [VM((members, sites), F32), VM((total, sites), F32), VM((total + 8, total), F32), VM((slots, own, total), F32)]
        + [dma((14,)), dma((6,)), dma((6,)), dma((2,)), dma((2,)), dma((4,)), dma((4,))]
        + [dma((2 * (n_ens - 1),))] * 2 + [dma((slots,))] * 4,
        compiler_params=pltpu.CompilerParams(collective_id=0, has_side_effects=True, vmem_limit_bytes=SPACE),
        name="step",
    )(*[pltpu.with_memory_space_constraint(x, pltpu.HBM) for x in
        (state, forcing, u_vel, v_vel, land, member_mode.reshape(1, members), theta.T, obs_index, values, sigma)])
    if not reduce_here:
        full = lax.psum(full, ("gx", "gy"))
    return out_lo, out_hi, full, th


def solve_kernel(members, full_ref, th_ref, out_ref, xs):
    total = full_ref.shape[1]
    blocks = total // 8
    n_ens, params = th_ref.shape[0], th_ref.shape[1]
    shape = (8, total)
    lane = lax.broadcasted_iota(jnp.int32, shape, 1)
    sub = lax.broadcasted_iota(jnp.int32, shape, 0)
    tht = jnp.concatenate([th_ref[e] for e in range(n_ens)], axis=1)
    spread = tht - jnp.mean(tht, axis=1, keepdims=True)
    xs[...] = jnp.zeros_like(xs)
    xs[0:params, :] = spread
    cols_of = xs[...].T
    A, R = [], []
    for k in range(blocks):
        rows = slice(8 * k, 8 * k + 8)
        A.append(full_ref[rows, :] + jnp.where(lane == sub + 8 * k, float(total - 1), 0.0))
        R.append(cols_of[rows])

    def splat(x):
        return jnp.broadcast_to(x, shape)

    def columns(x, k):
        return [jnp.take_along_axis(x, jnp.full(shape, 8 * k + j, jnp.int32), axis=1, mode="promise_in_bounds")
                for j in range(8)]

    def less(x, terms):
        terms = list(terms)
        while len(terms) > 1:
            terms = [sum(terms[t:t + 2][1:], terms[t]) for t in range(0, len(terms), 2)]
        return x - terms[0]

    for k in range(blocks):
        cols_k = columns(A[k], k)
        d = {(j, i): splat(cols_k[i][j:j + 1]) for j in range(8) for i in range(j, 8)}
        sets = [[splat(A[k][j:j + 1]) for j in range(8)]]
        if k == 0:
            sets.append([splat(R[k][j:j + 1]) for j in range(8)])
        pairs = {}
        for p in range(0, 8, 2):
            a, b, c = d[p, p], d[p, p + 1], d[p + 1, p + 1]
            r = 1.0 / (a * c - b * b)
            pairs[p] = a * r, b * r, c * r
            for i in range(p + 2, 8):
                m0 = (d[p, i] * c - d[p + 1, i] * b) * r
                m1 = (d[p + 1, i] * a - d[p, i] * b) * r
                for rs_ in sets:
                    rs_[i] = rs_[i] - (m0 * rs_[p] + m1 * rs_[p + 1])
                for q in range(i, 8):
                    d[i, q] = d[i, q] - (m0 * d[p, q] + m1 * d[p + 1, q])
        for p in reversed(range(0, 8, 2)):
            ar, br, cr = pairs[p]
            for rs_ in sets:
                y0, y1 = rs_[p], rs_[p + 1]
                if p < 6:
                    y0 = less(y0, [d[p, j] * rs_[j] for j in range(p + 2, 8)])
                    y1 = less(y1, [d[p + 1, j] * rs_[j] for j in range(p + 2, 8)])
                rs_[p], rs_[p + 1] = cr * y0 - br * y1, ar * y1 - br * y0

        def merge(rs_):
            x = rs_[7]
            for j in range(7):
                x = jnp.where(sub == j, rs_[j], x)
            return x

        for i in list(range(k + 1, blocks)) + list(range(k)):
            c = columns(A[i], k)
            A[i] = less(A[i], [c[j] * sets[0][j] for j in range(8)])
            if k == 0:
                R[i] = less(R[i], [c[j] * sets[1][j] for j in range(8)])
                A[i] = jnp.where(lane < 8, R[i], A[i])
        A[k] = merge(sets[0])
        if k == 0:
            A[k] = jnp.where(lane < 8, merge(sets[1]), A[k])
    for k in range(blocks):
        xs[8 * k:8 * k + 8, :] = A[k]
    x = xs[...].T[0:8]
    shift = jnp.sum(x * full_ref[total:total + 1, :], axis=1, keepdims=True)
    new = (jnp.mean(tht, axis=1, keepdims=True) + shift[0:params]) + float(total - 1) * x[0:params]
    ens = lax.axis_index("ens")
    for e in range(n_ens):
        @pl.when(ens == e)
        def _():
            out_ref[...] = new[:, e * members:(e + 1) * members]


def relay_kernel(members, full_ref, th_ref, lo_ref, hi_ref, out_ref, final_ref, xs, sem):
    depth, rows = lo_ref.shape[1], final_ref.shape[1]
    gives = [pltpu.make_async_copy(lo_ref, final_ref.at[:, 0:depth, :], sem.at[0]),
             pltpu.make_async_copy(hi_ref, final_ref.at[:, rows - depth:, :], sem.at[1])]
    for c in gives:
        c.start()
    solve_kernel(members, full_ref, th_ref, out_ref, xs)
    for c in gives:
        c.wait()


def solve(full, th, theta, lo, hi, shape):
    total = full.shape[1]
    out, final = pl.pallas_call(
        functools.partial(relay_kernel, theta.shape[0]),
        out_shape=[jax.ShapeDtypeStruct(theta.shape[::-1], F32), jax.ShapeDtypeStruct(shape, F32)],
        in_specs=[vspec()] * 4,
        out_specs=[vspec(), hspec()],
        scratch_shapes=[VM((total, total), F32), pltpu.SemaphoreType.DMA((2,))],
        compiler_params=pltpu.CompilerParams(vmem_limit_bytes=SMALL_SPACE),
        name="solve",
    )(full, th, lo, hi)
    return out.T, final


def local(mesh, state, u_vel, v_vel, land, forcing, member_mode, theta, obs_index, obs_values, obs_sigma):
    lo, hi, full, th = run_step(mesh, state, forcing, u_vel, v_vel, land, member_mode, theta, obs_index,
                                obs_values, obs_sigma)
    new_theta, final = solve(full, th, theta, lo, hi, state.shape)
    return final, new_theta


def solution(mesh):
    placed = (
        P("ens", "gy", "gx"),
        P("gy", "gx"),
        P("gy", "gx"),
        P("gy", "gx"),
        P(None, "gy", "gx"),
        P("ens"),
        P("ens", None),
        P("gy", "gx", None),
        P("gy", "gx", None),
        P("gy", "gx", None),
    )
    return jax.shard_map(
        functools.partial(local, mesh),
        mesh=mesh,
        in_specs=placed,
        out_specs=(P("ens", "gy", "gx"), P("ens", None)),
        check_vma=False,
    )
```

```python
import functools
import jax
import jax.numpy as jnp
from jax import lax
from jax.experimental import pallas as pl
from jax.experimental.pallas import tpu as pltpu
from jax.sharding import PartitionSpec as P

STEPS = 4
SPACE = 24 * 2**20
SMALL_SPACE = 12 * 2**20
DEPTH = 2 * STEPS
F32 = jnp.float32
I32 = jnp.int32
VM = pltpu.VMEM
MESH = pl.DeviceIdType.MESH
HIGH = lax.Precision.HIGHEST


def vspec():
    return pl.BlockSpec(memory_space=pltpu.VMEM)


def anyspec():
    return pl.BlockSpec(memory_space=pl.ANY)


def hspec():
    return pl.BlockSpec(memory_space=pltpu.HBM)


def flat(ref):
    return ref.reshape(ref.shape[0] * ref.shape[1], ref.shape[2])


def rdma(src, dst, send, recv, dev):
    return pltpu.make_async_remote_copy(src_ref=src, dst_ref=dst, send_sem=send, recv_sem=recv,
                                        device_id=dev, device_id_type=MESH)


def step_kernel(n_gx, n_gy, n_ens, reduce_here, owners,
                state_ref, forcing_ref, u_ref, v_ref, land_ref, mode_in, theta_in, index_in, val_in, sig_in,
                out_lo, out_hi, full_ref, th_ref,
                q_lo, q_hi, f_lo, f_hi, land_b, mode_ref, theta_ref, index_ref, val_ref, sig_ref,
                qt_ref, qb_ref, ft_ref, fb_ref, pack, corner, mid_ref, top_ref, bot_ref,
                Q, L, FO, US, H, LH, FH, UH, TH,
                obs_ref, obs_all, part, rs,
                load_sem, row_send, row_recv, gx_send, gx_recv, diag_send, diag_recv,
                ens_send, ens_recv, rs_send, rs_recv, ag_send, ag_recv):
    gx, gy, ens = lax.axis_index("gx"), lax.axis_index("gy"), lax.axis_index("ens")
    right, left = lax.rem(gx + 1, n_gx), lax.rem(gx + n_gx - 1, n_gx)
    has_up, has_down = gy > 0, gy < n_gy - 1
    up, down = jnp.maximum(gy - 1, 0), jnp.minimum(gy + 1, n_gy - 1)
    members, rows, cols = state_ref.shape
    patterns = forcing_ref.shape[0]
    fields = patterns + 3
    n_rows = rows + 2 * DEPTH
    n = n_gx * n_gy
    me = gy * n_gx + gx
    peers = [lax.rem(me + o, n) for o in range(1, n)] if reduce_here else []
    where = [{"gx": lax.rem(p, n_gx), "gy": lax.div(p, n_gx)} for p in peers]
    others = [lax.rem(ens + o, n_ens) for o in range(1, n_ens)]

    pairs = [(state_ref.at[:, 0:DEPTH, :], q_lo), (state_ref.at[:, rows - DEPTH:, :], q_hi)]
    for h, dst in ((0, f_lo), (rows - DEPTH, f_hi)):
        pairs += [(forcing_ref.at[:, h:h + DEPTH, :], dst.at[0:patterns]),
                  (u_ref.at[h:h + DEPTH, :], dst.at[patterns]), (v_ref.at[h:h + DEPTH, :], dst.at[patterns + 1])]
    pairs += [(land_ref, land_b), (mode_in, mode_ref), (theta_in, theta_ref), (index_in, index_ref),
              (val_in, val_ref), (sig_in, sig_ref)]
    loads = [pltpu.make_async_copy(s, d, load_sem.at[k]) for k, (s, d) in enumerate(pairs)]
    for c in loads:
        c.start()

    barrier = pltpu.get_barrier_semaphore()

    def greet(dev):
        pl.semaphore_signal(barrier, inc=1, device_id=dev, device_id_type=MESH)

    if reduce_here:
        order = sorted(range(1, n), key=lambda o: min(o, n - o))
        for o in order:
            greet(where[o - 1])
        expected = len(where)
    else:
        sides = 2
        expected = sides
        for dev in (right, left):
            greet({"gx": dev})
        for ok, dev in ((has_up, up), (has_down, down)):
            @pl.when(ok)
            def _():
                greet({"gy": dev})
                for other in (right, left):
                    greet({"gx": other, "gy": dev})
            expected = expected + (1 + sides) * ok.astype(I32)
    for p in others:
        greet({"ens": p})
    expected = expected + len(others)

    shape = (8, cols)
    lane = lax.broadcasted_iota(I32, shape, 1)
    sub = lax.broadcasted_iota(I32, shape, 0)
    low = jnp.bitwise_and(lane, 7)
    block0 = lane - low
    block = jnp.right_shift(lane, 3)
    blocks = cols // 8
    bits = [jnp.bitwise_and(lane, k) != 0 for k in (1, 2, 4)]
    first, last = lane < 8, lane >= cols - 8

    def roll(x, k):
        return pltpu.roll(x, k % cols, 1) if k % cols else x

    def gather(x, idx, axis):
        return jnp.take_along_axis(x, idx, axis=axis, mode="promise_in_bounds")

    def skew(xs):
        return [roll(x, v) for v, x in enumerate(xs)]

    def unskew(ys):
        for k, bit in zip((1, 2, 4), bits):
            ys = [jnp.where(bit, ys[(u + k) & 7], ys[u]) for u in range(8)]
        return [roll(ys[-c & 7], -c) for c in range(8)]

    slot = [0]
    queue = {}

    def at_slot(t, fn):
        if t <= slot[0]:
            fn()
        else:
            queue.setdefault(t, []).append(fn)

    def tick():
        slot[0] += 1
        for fn in queue.pop(slot[0], []):
            fn()

    def drain():
        while queue:
            tick()

    LAT = 3

    for c in loads:
        c.wait()
    for h, dst in ((0, f_lo), (rows - DEPTH, f_hi)):
        dst[patterns + 2] = (1 - land_b[h:h + DEPTH, :]).astype(F32)
        dst[fields:] = jnp.zeros((dst.shape[0] - fields, DEPTH, cols), F32)

    half_rows = DEPTH // 2
    near = [slice(0, half_rows), slice(half_rows, DEPTH)]
    downs = [rdma(f_hi.at[0:fields], ft_ref.at[0:fields], row_send.at[0], row_recv.at[0], {"gy": down})]
    ups = [rdma(f_lo.at[0:fields], fb_ref.at[0:fields], row_send.at[3], row_recv.at[3], {"gy": up})]
    for k, r in enumerate(near):
        downs.append(rdma(q_hi.at[:, r, :], qt_ref.at[:, r, :], row_send.at[1 + k], row_recv.at[1 + k], {"gy": down}))
        ups.append(rdma(q_lo.at[:, r, :], qb_ref.at[:, r, :], row_send.at[4 + k], row_recv.at[4 + k], {"gy": up}))
    dests = (right, left)
    fall = [rdma(corner.at[sd, 0], top_ref.at[sd], diag_send.at[sd], diag_recv.at[sd], {"gx": dests[sd], "gy": down})
            for sd in range(2)]
    rise = [rdma(corner.at[sd, 1], bot_ref.at[sd], diag_send.at[2 + sd], diag_recv.at[2 + sd],
                 {"gx": dests[sd], "gy": up}) for sd in range(2)]

    half_blocks = blocks // 2
    row_at = [2 * ((b - DEPTH // 2) % half_blocks) + (1 if (b - DEPTH // 2) % blocks >= half_blocks else 0)
              for b in range(blocks)]
    left_half = lane < cols // 2

    def pack_from(lo_ref, hi_ref, base):
        for g in range(lo_ref.shape[0] // 8):
            vals = []
            for r in range(rows):
                ref = flat(lo_ref if r < DEPTH else hi_ref)
                vals.append(ref[pl.ds(g * 8 * DEPTH + r % DEPTH, 8, stride=DEPTH), :])
            moved = [roll(jnp.where(left_half, vals[row_at[(b + 2) % blocks]], vals[row_at[b]]), 8 * b + 8)
                     for b in range(blocks)]
            hi, lo = moved[0], moved[0]
            for b in range(1, blocks):
                hi = jnp.where(block == b, moved[b], hi)
                lo = jnp.where(block == (b + 1) % blocks, moved[b], lo)
            packed.append((hi, lo))
            for sd in range(2):
                pack[sd, base + g * 8:base + g * 8 + 8, :] = packed[-1][sd]

    packed = []
    logical = [jnp.bitwise_and(block + sd, blocks - 1) for sd in range(2)]
    low_half = [jnp.bitwise_and(x, DEPTH // 2) == 0 for x in logical]
    pack_from(q_lo, q_hi, 0)
    pack_from(f_lo, f_hi, members)
    to_right = rdma(pack.at[0], mid_ref.at[0], gx_send.at[0], gx_recv.at[0], {"gx": right})
    to_left = rdma(pack.at[1], mid_ref.at[1], gx_send.at[1], gx_recv.at[1], {"gx": left})
    for p in range(len(packed) // 2):
        for sd in range(2):
            x, y = packed[2 * p][sd], roll(packed[2 * p + 1][sd], cols // 4)
            corner[sd, 0, p * 8:p * 8 + 8, :] = jnp.where(low_half[sd], x, y)
            corner[sd, 1, p * 8:p * 8 + 8, :] = jnp.where(low_half[sd], y, x)

    pl.semaphore_wait(barrier, expected)
    to_right.start()
    to_left.start()
    mine = pl.ds(pl.multiple_of(ens * members, members), members)
    th_copies, obs_copies = [], []
    early = members // 16 * 8
    for k, p in enumerate(others):
        th_copies.append(rdma(theta_ref, th_ref.at[ens], ens_send.at[3 * k], ens_recv.at[3 * k], {"ens": p}))
        for h, (at, size) in enumerate(((0, early), (early, members - early))):
            there = pl.ds(pl.multiple_of(ens * members + at, 8), size)
            obs_copies.append((h, rdma(obs_ref.at[at:at + size], obs_all.at[there], ens_send.at[3 * k + 1 + h],
                                       ens_recv.at[3 * k + 1 + h], {"ens": p})))
    for c in th_copies:
        c.start()

    @pl.when(has_down)
    def _():
        for c in fall + downs:
            c.start()

    @pl.when(has_up)
    def _():
        for c in rise + ups:
            c.start()

    TH[...] = jnp.zeros_like(TH)
    TH[0:theta_ref.shape[0], 0:members] = theta_ref[...]
    member = low * 8 + sub
    par = [gather(jnp.broadcast_to(TH[k:k + 1, :], shape), member, 1) for k in range(4)]
    diffuse = 0.05 * (1.0 + 0.5 * jnp.tanh(par[0]))
    hyper = 0.005 * (1.0 + 0.5 * jnp.tanh(par[1]))
    lap_gain = diffuse + 4.0 * hyper
    keep = 1.0 - 0.05 * (1.0 + 0.5 * jnp.tanh(par[2]))
    gain = par[3]
    mrow = jnp.concatenate([mode_ref[...], jnp.zeros((1, cols - members), I32)], axis=1)
    pattern_of = gather(jnp.broadcast_to(mrow, shape), member, 1)

    def spread(x):
        return [gather(x, block0 + c, 1) for c in range(8)]

    def place(i):
        return i & 1, (i >> 1) % blocks

    def edge_acc():
        return {"l": [jnp.zeros(shape, F32)] * 2, "r": [jnp.zeros(shape, F32)] * 2}

    def inward(acc, i, x0, x7):
        half, j = place(i)
        g = roll(jnp.where(last, x7, x0), 8 * j)

        def put():
            acc["l"][half] = jnp.where(block == j, g, acc["l"][half])
            acc["r"][half] = jnp.where(block == (j - 1) % blocks, g, acc["r"][half])
        at_slot(slot[0] + LAT, put)

    acc_q = edge_acc()

    def kept(ok, x):
        return x if ok is None else jnp.where(ok, x, 0.0)

    def enter_row(ref, k, base, ok):
        ref = flat(ref)
        ys = skew([kept(ok, ref[pl.ds(v * 8 * DEPTH + k, 8, stride=DEPTH), :]) for v in range(8)])

        def middle():
            os = unskew(ys)

            def end():
                for c in range(8):
                    Q[0, base + k, c] = os[c]
                inward(acc_q, base + k, os[0], os[7])
            at_slot(slot[0] + LAT, end)
        at_slot(slot[0] + LAT, middle)

    def enter_field_row(fr, k, base, ok):
        zs = spread(kept(ok, flat(fr)[pl.ds(k, 8, stride=DEPTH), :]))

        def end():
            for c in range(8):
                FO[base + k, c] = gain * gather(zs[c], pattern_of, 0)
        at_slot(slot[0] + LAT, end)

    def enter_planes(fr, base, ok):
        for f in range(3):
            x = kept(ok, flat(fr)[(patterns + f) * DEPTH:(patterns + f + 1) * DEPTH, :])
            x = x if f == 2 else 0.5 * x
            zs = spread(x)

            def end(f=f, zs=zs):
                for c, y in enumerate(zs):
                    US[f, c, base:base + DEPTH, :] = y
            at_slot(slot[0] + LAT, end)
            tick()

    def await_rows(k):
        @pl.when(has_down)
        def _():
            ups[k].wait_recv()

        @pl.when(has_up)
        def _():
            downs[k].wait_recv()

    for ref, fr, base in ((q_lo, f_lo, DEPTH), (q_hi, f_hi, rows)):
        for k in range(DEPTH):
            enter_row(ref, k, base, None)
            enter_field_row(fr, k, base, None)
            tick()
        enter_planes(fr, base, None)
    drain()

    await_rows(0)
    for fr, base, ok in ((ft_ref, 0, has_up), (fb_ref, DEPTH + rows, has_down)):
        for k in range(DEPTH):
            enter_field_row(fr, k, base, ok)
            tick()
        enter_planes(fr, base, ok)
    drain()
    for part_ in range(len(near)):
        await_rows(1 + part_)
        for ref, base, ok in ((qt_ref, 0, has_up), (qb_ref, DEPTH + rows, has_down)):
            for k in range(near[part_].start, near[part_].stop):
                enter_row(ref, k, base, ok)
                tick()
        drain()

    to_right.wait_recv()
    to_left.wait_recv()

    @pl.when(has_down)
    def _():
        for c in rise:
            c.wait_recv()

    @pl.when(has_up)
    def _():
        for c in fall:
            c.wait_recv()

    edge_ok, inner = [], []
    quarter = DEPTH // 2
    for side in range(2):
        ok = jnp.where(logical[side] < quarter, has_up.astype(I32),
                       jnp.where(logical[side] >= blocks - quarter, has_down.astype(I32), 1))
        edge_ok.append(ok > 0)
        inner.append((logical[side] >= quarter) & (logical[side] < blocks - quarter))

    def strip(side, g):
        p = g // 2
        mid = mid_ref[side, g * 8:g * 8 + 8, :]
        top, bot = top_ref[side, p * 8:p * 8 + 8, :], bot_ref[side, p * 8:p * 8 + 8, :]
        if g % 2:
            ends = roll(jnp.where(low_half[side], bot, top), -(cols // 4))
        else:
            ends = jnp.where(low_half[side], top, bot)
        even = jnp.where(inner[side], mid, roll(ends, cols // 2))
        odd = jnp.where(inner[side], roll(mid, cols // 2), ends)
        return [jnp.where(edge_ok[side], x, 0.0) for x in (even, odd)]

    scale = jnp.where(sub < 2, 0.5, 1.0)
    for side in range(2):
        both = [strip(side, v) for v in range(8)]
        cells = strip(side, members // 8)
        extra = strip(side, members // 8 + 1)
        for half in range(2):
            def start(side=side, half=half, both=both, cells=cells, extra=extra):
                ys = skew([b[half] for b in both])
                zs = spread(cells[half])
                ws = spread(scale * extra[half])

                def middle():
                    os = unskew(ys)
                    for c in range(8):
                        FH[side, c, half] = gain * gather(zs[c], pattern_of, 0)
                        UH[side, c, half] = ws[c]

                    def end():
                        for c in range(8):
                            H[0, side, c, half] = os[c]
                    at_slot(slot[0] + LAT, end)
                at_slot(slot[0] + LAT, middle)
            at_slot(slot[0] + 2, start)
            tick()
    drain()

    def masked(i, x):
        if i < DEPTH:
            return jnp.where(has_up, x, 0.0)
        if i >= DEPTH + rows:
            return jnp.where(has_down, x, 0.0)
        return x

    def across(x0, x7, get, i):
        half, j = place(i)
        f = roll(jnp.where(block == j, get(0, 7, half), get(1, 0, half)), -8 * j)
        return jnp.where(first, f, roll(x7, 8)), jnp.where(last, f, roll(x0, -8))

    def vertical(get, side, c):
        m, t = get(side, c, 0), get(side, c, 1)
        return (t, roll(t, 8)), (roll(m, -8), m)

    def halo_x(get, acc, side, c, half):
        if c > 0:
            xm = get(side, c - 1, half)
        else:
            xm = acc["r"][half] if side == 1 else jnp.zeros(shape, F32)
        if c < 7:
            xp = get(side, c + 1, half)
        else:
            xp = acc["l"][half] if side == 0 else jnp.zeros(shape, F32)
        return xm, xp

    def live(side, least):
        return range(least, 8) if side == 0 else range(0, 8 - least)

    def advance(s, acc_in):
        src, dst = s % 2, (s + 1) % 2
        lo, hi = 2 * s, n_rows - 2 * s
        final = s == STEPS - 1
        acc_l, acc_out = edge_acc(), edge_acc()
        qh = lambda side, c, half: H[src, side, c, half]
        lh = lambda side, c, half: LH[side, c, half]
        grads, adv, turn1, turn2, hv, lv = {}, {}, {}, {}, {}, {}
        lap_cells = [(0, 7), (1, 0)] if final else [(sd, c) for sd in range(2) for c in live(sd, lo + 1)]
        new_cells = [] if final else [(sd, c) for sd in range(2) for c in live(sd, lo + 2)]

        def halo_rolls():
            for sd, c in lap_cells:
                hv[sd, c] = vertical(qh, sd, c)

        def halo_lap():
            for sd, c in lap_cells:
                for half in range(2):
                    nxt, prv = hv[sd, c][half]
                    xm, xp = halo_x(qh, acc_in, sd, c, half)
                    lap = (nxt + prv) + (xp + xm) - 4.0 * qh(sd, c, half)
                    LH[sd, c, half] = jnp.where(edge_ok[sd], lap, 0.0)
                    if (sd, c) in new_cells:
                        grads[sd, c, half] = (UH[sd, c, half, 0:1] * (xp - xm) + UH[sd, c, half, 1:2] * (nxt - prv))

        def lap_rolls():
            for sd, c in new_cells:
                lv[sd, c] = vertical(lh, sd, c)

        def halo_new():
            for sd, c in new_cells:
                for half in range(2):
                    nxt, prv = lv[sd, c][half]
                    xm, xp = halo_x(lh, acc_l, sd, c, half)
                    mid = lh(sd, c, half)
                    around = (nxt + prv) + (xp + xm)
                    new = (keep * qh(sd, c, half) + (FH[sd, c, half] - grads[sd, c, half])
                           + (lap_gain * mid - hyper * around))
                    H[dst, sd, c, half] = new * UH[sd, c, half, 2:3]

        def turn_first(i):
            turn1[i] = across(Q[src, i, 0], Q[src, i, 7], qh, i)

        def first_pass(i):
            left, right = turn1.pop(i)
            row = [Q[src, i, c] for c in range(8)]
            laps = []
            for c in range(8):
                xm = row[c - 1] if c else left
                xp = row[c + 1] if c < 7 else right
                up_, dn = Q[src, i + 1, c], Q[src, i - 1, c]
                laps.append(masked(i, (up_ + dn) + (xp + xm) - 4.0 * row[c]))
                L[i, c] = laps[c]
                if lo + 2 <= i < hi - 2:
                    a = US[0, c, i:i + 1, :] * (xp - xm) + US[1, c, i:i + 1, :] * (up_ - dn)
                    adv[i, c] = keep * row[c] + (FO[i, c] - a)
            if not final:
                inward(acc_l, i, laps[0], laps[7])
            if lo + 2 <= i < hi - 2:
                turn2[i] = across(laps[0], laps[7], lh, i)

        def second_pass(i):
            left, right = turn2.pop(i)
            row = [L[i, c] for c in range(8)]
            outs = []
            for c in range(8):
                xm = row[c - 1] if c else left
                xp = row[c + 1] if c < 7 else right
                around = (L[i + 1, c] + L[i - 1, c]) + (xp + xm)
                new = (adv.pop((i, c)) + (lap_gain * row[c] - hyper * around)) * US[2, c, i:i + 1, :]
                outs.append(new)
                if not final:
                    Q[dst, i, c] = new
            if not final:
                inward(acc_out, i, outs[0], outs[7])
                return
            ys = skew(outs)

            def middle():
                xs = unskew(ys)

                def end():
                    r = i - DEPTH
                    ref = flat(out_lo if r < DEPTH else out_hi)
                    for v, x in enumerate(xs):
                        ref[pl.ds(v * 8 * DEPTH + r % DEPTH, 8, stride=DEPTH), :] = x
                at_slot(slot[0] + LAT, end)
            at_slot(slot[0] + LAT, middle)

        halo_rolls()
        for k in range(LAT):
            turn_first(lo + 1 + k)
        while any(fn.__name__ == "put" for fns in queue.values() for fn in fns):
            tick()
        halo_lap()
        lap_rolls()
        for i in range(lo + 1, hi - 1):
            if i + LAT < hi - 1:
                turn_first(i + LAT)
            first_pass(i)
            if lo + 2 <= i < hi - 2:
                at_slot(slot[0] + LAT, functools.partial(second_pass, i))
            tick()
        for _ in range(LAT):
            tick()
        if not final:
            halo_new()
        return acc_out

    acc = acc_q
    for s in range(STEPS):
        acc = advance(s, acc)
    drain()

    index = index_ref[0]
    col = jnp.bitwise_and(index, cols - 1)
    row = jnp.right_shift(index, cols.bit_length() - 1)
    hot = (lax.broadcasted_iota(I32, (cols, cols), 0) == col).astype(jnp.bfloat16)
    row_id = lax.broadcasted_iota(I32, (8, DEPTH, cols), 1)
    dot = functools.partial(jnp.dot, preferred_element_type=F32)
    for g in range(members // 8):
        found = []
        for h, ref in ((0, out_lo), (rows - DEPTH, out_hi)):
            x = flat(ref)[pl.ds(g * 8 * DEPTH, 8 * DEPTH), :]
            x1 = x.astype(jnp.bfloat16)
            rem = x - x1.astype(F32)
            x2 = rem.astype(jnp.bfloat16)
            x3 = (rem - x2.astype(F32)).astype(jnp.bfloat16)
            picked = dot(x1, hot) + (dot(x2, hot) + dot(x3, hot))
            found.append(jnp.where(row_id + h == row[None], picked.reshape(8, DEPTH, cols), 0.0))
        obs_ref[pl.ds(g * 8, 8), :] = jnp.sum(found[0] + found[1], axis=1)
        for h, c in obs_copies:
            if (g + 1) * 8 == (early, members)[h]:
                c.start()

    obs_all[mine, :] = obs_ref[...]
    th_ref[ens] = theta_ref[...]
    for _, c in obs_copies:
        c.wait()

    x = obs_all[...]
    mean = jnp.mean(x, axis=0, keepdims=True)
    inv = 1.0 / sig_ref[0]
    anom = (x - mean) * inv
    d = jnp.broadcast_to((val_ref[0] - mean) * inv, (8, x.shape[1]))
    total = x.shape[0]
    gram = lax.dot_general(jnp.concatenate([anom, d], axis=0), anom, (((1,), (1,)), ((), ())),
                           preferred_element_type=F32, precision=HIGH)

    def finish():
        for c in (to_right, to_left):
            c.wait_send()
        for ok, copies in ((has_down, fall + downs), (has_up, rise + ups)):
            @pl.when(ok)
            def _():
                for c in copies:
                    c.wait_send()
        for c in th_copies:
            c.wait()

    if not reduce_here:
        full_ref[...] = gram
        finish()
        return
    part[...] = gram
    own = total // len(owners)
    spans = [pl.ds(k * own, own + (8 if k == len(owners) - 1 else 0)) for k in range(len(owners))]
    rank = [oy * n_gx + ox for ox, oy in owners]

    def to_owner(k, slot_):
        return rdma(part.at[spans[k]], rs.at[slot_, 0:spans[k].size], rs_send.at[k], rs_recv.at[0],
                    {"gx": owners[k][0], "gy": owners[k][1]})

    def all_slots(k):
        return rs.at[:, 0:spans[k].size]

    def arrivals(k):
        return rdma(all_slots(k), all_slots(k), rs_send.at[k], rs_recv.at[0],
                    {"gx": owners[k][0], "gy": owners[k][1]})

    def departures(k):
        return rdma(all_slots(k), all_slots(k), ag_send.at[0], ag_recv.at[k], where[0])

    def from_owner(k, j):
        return rdma(full_ref.at[spans[k]], full_ref.at[spans[k]], ag_send.at[0], ag_recv.at[k], where[j])

    for k in range(len(owners)):
        @pl.when(me != rank[k])
        def _():
            to_owner(k, lax.rem(me + (n - 1 - rank[k]), n)).start()
    for k in range(len(owners)):
        @pl.when(me == rank[k])
        def _():
            arrivals(k).wait_recv()
            terms = [part[spans[k], :]] + [rs[p, 0:spans[k].size, :] for p in range(n - 1)]
            while len(terms) > 1:
                terms = [sum(terms[t:t + 2][1:], terms[t]) for t in range(0, len(terms), 2)]
            full_ref[spans[k], :] = terms[0]
            for j in range(len(where)):
                from_owner(k, j).start()
    for k in range(len(owners)):
        @pl.when(me != rank[k])
        def _():
            to_owner(k, 0).wait_send()
    finish()
    for k in range(len(owners)):
        @pl.when(me != rank[k])
        def _():
            from_owner(k, 0).wait_recv()

        @pl.when(me == rank[k])
        def _():
            departures(k).wait_send()


def run_step(mesh, state, forcing, u_vel, v_vel, land, member_mode, theta, obs_index, values, sigma):
    n_gx, n_gy, n_ens = mesh.shape["gx"], mesh.shape["gy"], mesh.shape["ens"]
    members, rows, cols = state.shape
    patterns = forcing.shape[0]
    sites = obs_index.shape[-1]
    params = theta.shape[1]
    nf = -(-(patterns + 3) // 8) * 8
    strips = members + nf
    n_rows = rows + 2 * DEPTH
    total = members * n_ens
    n = n_gx * n_gy
    owners = [(ox, oy) for oy in range(1, n_gy, 2) for ox in sorted({max(n_gx // 2 - 1, 0), n_gx // 2})]
    reduce_here = 0 < n <= 32 and len(owners) > 0 and total % (8 * len(owners)) == 0
    own = total // len(owners) + 8 if reduce_here else 8
    slots = n - 1 if reduce_here else 1
    sums = len(owners) if reduce_here else 1
    sds = jax.ShapeDtypeStruct
    dma = pltpu.SemaphoreType.DMA
    reg = (8, cols)
    out_lo, out_hi, full, th = pl.pallas_call(
        functools.partial(step_kernel, n_gx, n_gy, n_ens, reduce_here, owners),
        out_shape=[sds((members, DEPTH, cols), F32)] * 2 + [sds((total + 8, total), F32),
                   sds((n_ens, params, members), F32)],
        in_specs=[hspec()] * 10,
        out_specs=[vspec()] * 4,
        scratch_shapes=[VM((members, DEPTH, cols), F32)] * 2 + [VM((nf, DEPTH, cols), F32)] * 2
        + [VM((rows, cols), I32), VM((1, members), I32), VM((params, members), F32), VM((1, 1, sites), I32),
           VM((1, 1, sites), F32), VM((1, 1, sites), F32)]
        + [VM((members, DEPTH, cols), F32)] * 2 + [VM((nf, DEPTH, cols), F32)] * 2
        + [VM((2, strips, cols), F32), VM((2, 2, strips // 2, cols), F32), VM((2, strips, cols), F32)]
        + [VM((2, strips // 2, cols), F32)] * 2
        + [VM((2, n_rows, 8) + reg, F32), VM((n_rows, 8) + reg, F32), VM((n_rows, 8) + reg, F32),
           VM((3, 8, n_rows, cols), F32),
           VM((2, 2, 8, 2) + reg, F32), VM((2, 8, 2) + reg, F32), VM((2, 8, 2) + reg, F32),
           VM((2, 8, 2) + reg, F32), VM(reg, F32)]
        + [VM((members, sites), F32), VM((total, sites), F32), VM((total + 8, total), F32), VM((slots, own, total), F32)]
        + [dma((14,)), dma((6,)), dma((6,)), dma((2,)), dma((2,)), dma((4,)), dma((4,))]
        + [dma((3 * (n_ens - 1),))] * 2 + [dma((sums,)), dma((1,)), dma((1,)), dma((sums,))],
        compiler_params=pltpu.CompilerParams(collective_id=0, has_side_effects=True, vmem_limit_bytes=SPACE),
        name="step",
    )(*[pltpu.with_memory_space_constraint(x, pltpu.HBM) for x in
        (state, forcing, u_vel, v_vel, land, member_mode.reshape(1, members), theta.T, obs_index, values, sigma)])
    if not reduce_here:
        full = lax.psum(full, ("gx", "gy"))
    return out_lo, out_hi, full, th


def solve_kernel(members, full_ref, th_ref, out_ref, xs):
    total = full_ref.shape[1]
    blocks = total // 8
    n_ens, params = th_ref.shape[0], th_ref.shape[1]
    shape = (8, total)
    lane = lax.broadcasted_iota(jnp.int32, shape, 1)
    sub = lax.broadcasted_iota(jnp.int32, shape, 0)
    tht = jnp.concatenate([th_ref[e] for e in range(n_ens)], axis=1)
    spread = tht - jnp.mean(tht, axis=1, keepdims=True)
    xs[...] = jnp.zeros_like(xs)
    xs[0:params, :] = spread
    cols_of = xs[...].T
    A, R = [], []
    for k in range(blocks):
        rows = slice(8 * k, 8 * k + 8)
        A.append(full_ref[rows, :] + jnp.where(lane == sub + 8 * k, float(total - 1), 0.0))
        R.append(cols_of[rows])

    def splat(x):
        return jnp.broadcast_to(x, shape)

    def columns(x, k):
        return [jnp.take_along_axis(x, jnp.full(shape, 8 * k + j, jnp.int32), axis=1, mode="promise_in_bounds")
                for j in range(8)]

    def less(x, terms):
        terms = list(terms)
        while len(terms) > 1:
            terms = [sum(terms[t:t + 2][1:], terms[t]) for t in range(0, len(terms), 2)]
        return x - terms[0]

    for k in range(blocks):
        cols_k = columns(A[k], k)
        d = {(j, i): splat(cols_k[i][j:j + 1]) for j in range(8) for i in range(j, 8)}
        sets = [[splat(A[k][j:j + 1]) for j in range(8)]]
        if k == 0:
            sets.append([splat(R[k][j:j + 1]) for j in range(8)])
        pairs = {}
        for p in range(0, 8, 2):
            a, b, c = d[p, p], d[p, p + 1], d[p + 1, p + 1]
            r = 1.0 / (a * c - b * b)
            pairs[p] = a * r, b * r, c * r
            for i in range(p + 2, 8):
                m0 = (d[p, i] * c - d[p + 1, i] * b) * r
                m1 = (d[p + 1, i] * a - d[p, i] * b) * r
                for rs_ in sets:
                    rs_[i] = rs_[i] - (m0 * rs_[p] + m1 * rs_[p + 1])
                for q in range(i, 8):
                    d[i, q] = d[i, q] - (m0 * d[p, q] + m1 * d[p + 1, q])
        for p in reversed(range(0, 8, 2)):
            ar, br, cr = pairs[p]
            for rs_ in sets:
                y0, y1 = rs_[p], rs_[p + 1]
                if p < 6:
                    y0 = less(y0, [d[p, j] * rs_[j] for j in range(p + 2, 8)])
                    y1 = less(y1, [d[p + 1, j] * rs_[j] for j in range(p + 2, 8)])
                rs_[p], rs_[p + 1] = cr * y0 - br * y1, ar * y1 - br * y0

        def merge(rs_):
            x = rs_[7]
            for j in range(7):
                x = jnp.where(sub == j, rs_[j], x)
            return x

        for i in list(range(k + 1, blocks)) + list(range(k)):
            c = columns(A[i], k)
            A[i] = less(A[i], [c[j] * sets[0][j] for j in range(8)])
            if k == 0:
                R[i] = less(R[i], [c[j] * sets[1][j] for j in range(8)])
                A[i] = jnp.where(lane < 8, R[i], A[i])
        A[k] = merge(sets[0])
        if k == 0:
            A[k] = jnp.where(lane < 8, merge(sets[1]), A[k])
    for k in range(blocks):
        xs[8 * k:8 * k + 8, :] = A[k]
    x = xs[...].T[0:8]
    shift = jnp.sum(x * full_ref[total:total + 1, :], axis=1, keepdims=True)
    new = (jnp.mean(tht, axis=1, keepdims=True) + shift[0:params]) + float(total - 1) * x[0:params]
    ens = lax.axis_index("ens")
    for e in range(n_ens):
        @pl.when(ens == e)
        def _():
            out_ref[...] = new[:, e * members:(e + 1) * members]


def relay_kernel(members, full_ref, th_ref, lo_ref, hi_ref, out_ref, final_ref, xs, sem):
    depth, rows = lo_ref.shape[1], final_ref.shape[1]
    gives = [pltpu.make_async_copy(lo_ref, final_ref.at[:, 0:depth, :], sem.at[0]),
             pltpu.make_async_copy(hi_ref, final_ref.at[:, rows - depth:, :], sem.at[1])]
    for c in gives:
        c.start()
    solve_kernel(members, full_ref, th_ref, out_ref, xs)
    for c in gives:
        c.wait()


def solve(full, th, theta, lo, hi, shape):
    total = full.shape[1]
    out, final = pl.pallas_call(
        functools.partial(relay_kernel, theta.shape[0]),
        out_shape=[jax.ShapeDtypeStruct(theta.shape[::-1], F32), jax.ShapeDtypeStruct(shape, F32)],
        in_specs=[vspec()] * 4,
        out_specs=[vspec(), hspec()],
        scratch_shapes=[VM((total, total), F32), pltpu.SemaphoreType.DMA((2,))],
        compiler_params=pltpu.CompilerParams(vmem_limit_bytes=SMALL_SPACE),
        name="solve",
    )(full, th, lo, hi)
    return out.T, final


def local(mesh, state, u_vel, v_vel, land, forcing, member_mode, theta, obs_index, obs_values, obs_sigma):
    lo, hi, full, th = run_step(mesh, state, forcing, u_vel, v_vel, land, member_mode, theta, obs_index,
                                obs_values, obs_sigma)
    new_theta, final = solve(full, th, theta, lo, hi, state.shape)
    return final, new_theta


def solution(mesh):
    placed = (
        P("ens", "gy", "gx"),
        P("gy", "gx"),
        P("gy", "gx"),
        P("gy", "gx"),
        P(None, "gy", "gx"),
        P("ens"),
        P("ens", None),
        P("gy", "gx", None),
        P("gy", "gx", None),
        P("gy", "gx", None),
    )
    return jax.shard_map(
        functools.partial(local, mesh),
        mesh=mesh,
        in_specs=placed,
        out_specs=(P("ens", "gy", "gx"), P("ens", None)),
        check_vma=False,
    )
```

```python
import functools
import jax
import jax.numpy as jnp
from jax import lax
from jax.experimental import pallas as pl
from jax.experimental.pallas import tpu as pltpu
from jax.sharding import PartitionSpec as P

STEPS = 4
SPACE = 24 * 2**20
SMALL_SPACE = 12 * 2**20
DEPTH = 2 * STEPS
F32 = jnp.float32
I32 = jnp.int32
VM = pltpu.VMEM
MESH = pl.DeviceIdType.MESH
HIGH = lax.Precision.HIGHEST


def vspec():
    return pl.BlockSpec(memory_space=pltpu.VMEM)


def anyspec():
    return pl.BlockSpec(memory_space=pl.ANY)


def hspec():
    return pl.BlockSpec(memory_space=pltpu.HBM)


def flat(ref):
    return ref.reshape(ref.shape[0] * ref.shape[1], ref.shape[2])


def rdma(src, dst, send, recv, dev):
    return pltpu.make_async_remote_copy(src_ref=src, dst_ref=dst, send_sem=send, recv_sem=recv,
                                        device_id=dev, device_id_type=MESH)


def folded(total):
    return total * 5 // 8 + 8


def share(size, count):
    cuts = [8 * (size // 8 * k // count) for k in range(count + 1)]
    return [pl.ds(a, b - a) for a, b in zip(cuts, cuts[1:])]


def fold(g, total):
    q = total // 4
    lane = lax.broadcasted_iota(I32, (8, total), 1)
    rows_of = lambda r: g[r:r + 8]
    out = [rows_of(r) for r in range(0, q, 8)]
    for r in range(0, q, 8):
        out.append(jnp.where(lane < q, pltpu.roll(rows_of(3 * q + r), q, 1), rows_of(q + r)))
    for r in range(0, q // 2, 8):
        out.append(jnp.where(lane < 2 * q, pltpu.roll(rows_of(2 * q + q // 2 + r), 2 * q, 1), rows_of(2 * q + r)))
    return out + [rows_of(total)]


def unfold(ref, total):
    q = total // 4
    lane = lax.broadcasted_iota(I32, (8, total), 1)
    rows_of = lambda r: ref[r:r + 8, :]
    top = [rows_of(r) for r in range(0, q, 8)]
    second = [rows_of(q + r) for r in range(0, q, 8)]
    third = [rows_of(2 * q + r) for r in range(0, q // 2, 8)]
    upper = top + second + third + [pltpu.roll(x, 2 * q, 1) for x in third] + [pltpu.roll(x, 3 * q, 1) for x in second]
    mirror = jnp.concatenate(upper, axis=0).T
    return [jnp.where(lane < 8 * k // q * q, mirror[8 * k:8 * k + 8], x) for k, x in enumerate(upper)]


def step_kernel(n_gx, n_gy, n_ens, reduce_here, owners,
                state_ref, forcing_ref, u_ref, v_ref, land_ref, mode_in, theta_in, index_in, val_in, sig_in,
                out_lo, out_hi, full_ref, th_ref,
                q_lo, q_hi, f_lo, f_hi, land_b, mode_ref, theta_ref, index_ref, val_ref, sig_ref,
                qt_ref, qb_ref, ft_ref, fb_ref, pack, corner, mid_ref, top_ref, bot_ref,
                Q, L, FO, US, H, LH, FH, UH, TH,
                obs_ref, obs_all, part, rs,
                load_sem, row_send, row_recv, gx_send, gx_recv, diag_send, diag_recv,
                ens_send, ens_recv, rs_send, rs_recv, ag_send, ag_recv):
    gx, gy, ens = lax.axis_index("gx"), lax.axis_index("gy"), lax.axis_index("ens")
    right, left = lax.rem(gx + 1, n_gx), lax.rem(gx + n_gx - 1, n_gx)
    has_up, has_down = gy > 0, gy < n_gy - 1
    up, down = jnp.maximum(gy - 1, 0), jnp.minimum(gy + 1, n_gy - 1)
    members, rows, cols = state_ref.shape
    patterns = forcing_ref.shape[0]
    fields = patterns + 3
    n_rows = rows + 2 * DEPTH
    n = n_gx * n_gy
    me = gy * n_gx + gx
    peers = [lax.rem(me + o, n) for o in range(1, n)] if reduce_here else []
    where = [{"gx": lax.rem(p, n_gx), "gy": lax.div(p, n_gx)} for p in peers]
    others = [lax.rem(ens + o, n_ens) for o in range(1, n_ens)]

    pairs = [(state_ref.at[:, 0:DEPTH, :], q_lo), (state_ref.at[:, rows - DEPTH:, :], q_hi)]
    for h, dst in ((0, f_lo), (rows - DEPTH, f_hi)):
        pairs += [(forcing_ref.at[:, h:h + DEPTH, :], dst.at[0:patterns]),
                  (u_ref.at[h:h + DEPTH, :], dst.at[patterns]), (v_ref.at[h:h + DEPTH, :], dst.at[patterns + 1])]
    pairs += [(land_ref, land_b), (mode_in, mode_ref), (theta_in, theta_ref), (index_in, index_ref),
              (val_in, val_ref), (sig_in, sig_ref)]
    loads = [pltpu.make_async_copy(s, d, load_sem.at[k]) for k, (s, d) in enumerate(pairs)]
    for c in loads:
        c.start()

    barrier = pltpu.get_barrier_semaphore()

    def greet(dev):
        pl.semaphore_signal(barrier, inc=1, device_id=dev, device_id_type=MESH)

    if reduce_here:
        order = sorted(range(1, n), key=lambda o: min(o, n - o))
        for o in order:
            greet(where[o - 1])
        expected = len(where)
    else:
        sides = 2
        expected = sides
        for dev in (right, left):
            greet({"gx": dev})
        for ok, dev in ((has_up, up), (has_down, down)):
            @pl.when(ok)
            def _():
                greet({"gy": dev})
                for other in (right, left):
                    greet({"gx": other, "gy": dev})
            expected = expected + (1 + sides) * ok.astype(I32)
    for p in others:
        greet({"ens": p})
    expected = expected + len(others)

    shape = (8, cols)
    lane = lax.broadcasted_iota(I32, shape, 1)
    sub = lax.broadcasted_iota(I32, shape, 0)
    low = jnp.bitwise_and(lane, 7)
    block0 = lane - low
    block = jnp.right_shift(lane, 3)
    blocks = cols // 8
    bits = [jnp.bitwise_and(lane, k) != 0 for k in (1, 2, 4)]
    first, last = lane < 8, lane >= cols - 8

    def roll(x, k):
        return pltpu.roll(x, k % cols, 1) if k % cols else x

    def gather(x, idx, axis):
        return jnp.take_along_axis(x, idx, axis=axis, mode="promise_in_bounds")

    def skew(xs):
        return [roll(x, v) for v, x in enumerate(xs)]

    def unskew(ys):
        for k, bit in zip((1, 2, 4), bits):
            ys = [jnp.where(bit, ys[(u + k) & 7], ys[u]) for u in range(8)]
        return [roll(ys[-c & 7], -c) for c in range(8)]

    slot = [0]
    queue = {}

    def at_slot(t, fn):
        if t <= slot[0]:
            fn()
        else:
            queue.setdefault(t, []).append(fn)

    def tick():
        slot[0] += 1
        for fn in queue.pop(slot[0], []):
            fn()

    def drain():
        while queue:
            tick()

    LAT = 5

    for c in loads:
        c.wait()
    for h, dst in ((0, f_lo), (rows - DEPTH, f_hi)):
        dst[patterns + 2] = (1 - land_b[h:h + DEPTH, :]).astype(F32)
        dst[fields:] = jnp.zeros((dst.shape[0] - fields, DEPTH, cols), F32)

    half_rows = DEPTH // 2
    near = [slice(0, half_rows), slice(half_rows, DEPTH)]
    downs = [rdma(f_hi.at[0:fields], ft_ref.at[0:fields], row_send.at[0], row_recv.at[0], {"gy": down})]
    ups = [rdma(f_lo.at[0:fields], fb_ref.at[0:fields], row_send.at[3], row_recv.at[3], {"gy": up})]
    for k, r in enumerate(near):
        downs.append(rdma(q_hi.at[:, r, :], qt_ref.at[:, r, :], row_send.at[1 + k], row_recv.at[1 + k], {"gy": down}))
        ups.append(rdma(q_lo.at[:, r, :], qb_ref.at[:, r, :], row_send.at[4 + k], row_recv.at[4 + k], {"gy": up}))
    dests = (right, left)
    fall = [rdma(corner.at[sd, 0], top_ref.at[sd], diag_send.at[sd], diag_recv.at[sd], {"gx": dests[sd], "gy": down})
            for sd in range(2)]
    rise = [rdma(corner.at[sd, 1], bot_ref.at[sd], diag_send.at[2 + sd], diag_recv.at[2 + sd],
                 {"gx": dests[sd], "gy": up}) for sd in range(2)]

    half_blocks = blocks // 2
    row_at = [2 * ((b - DEPTH // 2) % half_blocks) + (1 if (b - DEPTH // 2) % blocks >= half_blocks else 0)
              for b in range(blocks)]
    left_half = lane < cols // 2

    def pack_from(lo_ref, hi_ref, base):
        for g in range(lo_ref.shape[0] // 8):
            vals = []
            for r in range(rows):
                ref = flat(lo_ref if r < DEPTH else hi_ref)
                vals.append(ref[pl.ds(g * 8 * DEPTH + r % DEPTH, 8, stride=DEPTH), :])
            moved = [roll(jnp.where(left_half, vals[row_at[(b + 2) % blocks]], vals[row_at[b]]), 8 * b + 8)
                     for b in range(blocks)]
            hi, lo = moved[0], moved[0]
            for b in range(1, blocks):
                hi = jnp.where(block == b, moved[b], hi)
                lo = jnp.where(block == (b + 1) % blocks, moved[b], lo)
            packed.append((hi, lo))
            for sd in range(2):
                pack[sd, base + g * 8:base + g * 8 + 8, :] = packed[-1][sd]

    packed = []
    logical = [jnp.bitwise_and(block + sd, blocks - 1) for sd in range(2)]
    low_half = [jnp.bitwise_and(x, DEPTH // 2) == 0 for x in logical]
    pack_from(q_lo, q_hi, 0)
    pack_from(f_lo, f_hi, members)
    to_right = rdma(pack.at[0], mid_ref.at[0], gx_send.at[0], gx_recv.at[0], {"gx": right})
    to_left = rdma(pack.at[1], mid_ref.at[1], gx_send.at[1], gx_recv.at[1], {"gx": left})
    for p in range(len(packed) // 2):
        for sd in range(2):
            x, y = packed[2 * p][sd], roll(packed[2 * p + 1][sd], cols // 4)
            corner[sd, 0, p * 8:p * 8 + 8, :] = jnp.where(low_half[sd], x, y)
            corner[sd, 1, p * 8:p * 8 + 8, :] = jnp.where(low_half[sd], y, x)

    pl.semaphore_wait(barrier, expected)
    to_right.start()
    to_left.start()
    mine = pl.ds(pl.multiple_of(ens * members, members), members)
    th_copies, obs_copies = [], []
    early = members // 16 * 8
    for k, p in enumerate(others):
        th_copies.append(rdma(theta_ref, th_ref.at[ens], ens_send.at[3 * k], ens_recv.at[3 * k], {"ens": p}))
        for h, (at, size) in enumerate(((0, early), (early, members - early))):
            there = pl.ds(pl.multiple_of(ens * members + at, 8), size)
            obs_copies.append((h, rdma(obs_ref.at[at:at + size], obs_all.at[there], ens_send.at[3 * k + 1 + h],
                                       ens_recv.at[3 * k + 1 + h], {"ens": p})))
    for c in th_copies:
        c.start()

    @pl.when(has_down)
    def _():
        for c in fall + downs:
            c.start()

    @pl.when(has_up)
    def _():
        for c in rise + ups:
            c.start()

    TH[...] = jnp.zeros_like(TH)
    TH[0:theta_ref.shape[0], 0:members] = theta_ref[...]
    member = low * 8 + sub
    par = [gather(jnp.broadcast_to(TH[k:k + 1, :], shape), member, 1) for k in range(4)]
    diffuse = 0.05 * (1.0 + 0.5 * jnp.tanh(par[0]))
    hyper = 0.005 * (1.0 + 0.5 * jnp.tanh(par[1]))
    lap_gain = diffuse + 4.0 * hyper
    keep = 1.0 - 0.05 * (1.0 + 0.5 * jnp.tanh(par[2]))
    gain = par[3]
    mrow = jnp.concatenate([mode_ref[...], jnp.zeros((1, cols - members), I32)], axis=1)
    pattern_of = gather(jnp.broadcast_to(mrow, shape), member, 1)

    def spread(x):
        return [gather(x, block0 + c, 1) for c in range(8)]

    def place(i):
        return i & 1, (i >> 1) % blocks

    def edge_acc():
        return {"l": [jnp.zeros(shape, F32)] * 2, "r": [jnp.zeros(shape, F32)] * 2}

    def inward(acc, i, x0, x7):
        half, j = place(i)
        g = roll(jnp.where(last, x7, x0), 8 * j)

        def put():
            acc["l"][half] = jnp.where(block == j, g, acc["l"][half])
            acc["r"][half] = jnp.where(block == (j - 1) % blocks, g, acc["r"][half])
        at_slot(slot[0] + LAT, put)

    acc_q = edge_acc()

    def kept(ok, x):
        return x if ok is None else jnp.where(ok, x, 0.0)

    def enter_row(ref, k, base, ok):
        ref = flat(ref)
        ys = skew([kept(ok, ref[pl.ds(v * 8 * DEPTH + k, 8, stride=DEPTH), :]) for v in range(8)])

        def middle():
            os = unskew(ys)

            def end():
                for c in range(8):
                    Q[0, base + k, c] = os[c]
                inward(acc_q, base + k, os[0], os[7])
            at_slot(slot[0] + LAT, end)
        at_slot(slot[0] + LAT, middle)

    def enter_field_row(fr, k, base, ok):
        zs = spread(kept(ok, flat(fr)[pl.ds(k, 8, stride=DEPTH), :]))

        def end():
            for c in range(8):
                FO[base + k, c] = gain * gather(zs[c], pattern_of, 0)
        at_slot(slot[0] + LAT, end)

    def enter_planes(fr, base, ok):
        for f in range(3):
            x = kept(ok, flat(fr)[(patterns + f) * DEPTH:(patterns + f + 1) * DEPTH, :])
            x = x if f == 2 else 0.5 * x
            zs = spread(x)

            def end(f=f, zs=zs):
                for c, y in enumerate(zs):
                    US[f, c, base:base + DEPTH, :] = y
            at_slot(slot[0] + LAT, end)
            tick()

    def await_rows(k):
        @pl.when(has_down)
        def _():
            ups[k].wait_recv()

        @pl.when(has_up)
        def _():
            downs[k].wait_recv()

    for ref, fr, base in ((q_lo, f_lo, DEPTH), (q_hi, f_hi, rows)):
        for k in range(DEPTH):
            enter_row(ref, k, base, None)
            enter_field_row(fr, k, base, None)
            tick()
        enter_planes(fr, base, None)
    drain()

    await_rows(0)
    for fr, base, ok in ((ft_ref, 0, has_up), (fb_ref, DEPTH + rows, has_down)):
        for k in range(DEPTH):
            enter_field_row(fr, k, base, ok)
            tick()
        enter_planes(fr, base, ok)
    drain()
    for part_ in range(len(near)):
        await_rows(1 + part_)
        for ref, base, ok in ((qt_ref, 0, has_up), (qb_ref, DEPTH + rows, has_down)):
            for k in range(near[part_].start, near[part_].stop):
                enter_row(ref, k, base, ok)
                tick()
        drain()

    to_right.wait_recv()
    to_left.wait_recv()

    @pl.when(has_down)
    def _():
        for c in rise:
            c.wait_recv()

    @pl.when(has_up)
    def _():
        for c in fall:
            c.wait_recv()

    edge_ok, inner = [], []
    quarter = DEPTH // 2
    for side in range(2):
        ok = jnp.where(logical[side] < quarter, has_up.astype(I32),
                       jnp.where(logical[side] >= blocks - quarter, has_down.astype(I32), 1))
        edge_ok.append(ok > 0)
        inner.append((logical[side] >= quarter) & (logical[side] < blocks - quarter))

    def strip(side, g):
        p = g // 2
        mid = mid_ref[side, g * 8:g * 8 + 8, :]
        top, bot = top_ref[side, p * 8:p * 8 + 8, :], bot_ref[side, p * 8:p * 8 + 8, :]
        if g % 2:
            ends = roll(jnp.where(low_half[side], bot, top), -(cols // 4))
        else:
            ends = jnp.where(low_half[side], top, bot)
        even = jnp.where(inner[side], mid, roll(ends, cols // 2))
        odd = jnp.where(inner[side], roll(mid, cols // 2), ends)
        return [jnp.where(edge_ok[side], x, 0.0) for x in (even, odd)]

    scale = jnp.where(sub < 2, 0.5, 1.0)
    for side in range(2):
        both = [strip(side, v) for v in range(8)]
        cells = strip(side, members // 8)
        extra = strip(side, members // 8 + 1)
        for half in range(2):
            def start(side=side, half=half, both=both, cells=cells, extra=extra):
                ys = skew([b[half] for b in both])
                zs = spread(cells[half])
                ws = spread(scale * extra[half])

                def middle():
                    os = unskew(ys)
                    for c in range(8):
                        FH[side, c, half] = gain * gather(zs[c], pattern_of, 0)
                        UH[side, c, half] = ws[c]

                    def end():
                        for c in range(8):
                            H[0, side, c, half] = os[c]
                    at_slot(slot[0] + LAT, end)
                at_slot(slot[0] + LAT, middle)
            at_slot(slot[0] + 2, start)
            tick()
    drain()

    def masked(i, x):
        if i < DEPTH:
            return jnp.where(has_up, x, 0.0)
        if i >= DEPTH + rows:
            return jnp.where(has_down, x, 0.0)
        return x

    def across(x0, x7, get, i):
        half, j = place(i)
        f = roll(jnp.where(block == j, get(0, 7, half), get(1, 0, half)), -8 * j)
        return jnp.where(first, f, roll(x7, 8)), jnp.where(last, f, roll(x0, -8))

    def vertical(get, side, c):
        m, t = get(side, c, 0), get(side, c, 1)
        return (t, roll(t, 8)), (roll(m, -8), m)

    def halo_x(get, acc, side, c, half):
        if c > 0:
            xm = get(side, c - 1, half)
        else:
            xm = acc["r"][half] if side == 1 else jnp.zeros(shape, F32)
        if c < 7:
            xp = get(side, c + 1, half)
        else:
            xp = acc["l"][half] if side == 0 else jnp.zeros(shape, F32)
        return xm, xp

    def live(side, least):
        return range(least, 8) if side == 0 else range(0, 8 - least)

    def advance(s, acc_in):
        src, dst = s % 2, (s + 1) % 2
        lo, hi = 2 * s, n_rows - 2 * s
        final = s == STEPS - 1
        acc_l, acc_out = edge_acc(), edge_acc()
        qh = lambda side, c, half: H[src, side, c, half]
        lh = lambda side, c, half: LH[side, c, half]
        grads, adv, turn1, turn2, hv, lv = {}, {}, {}, {}, {}, {}
        lap_cells = [(0, 7), (1, 0)] if final else [(sd, c) for sd in range(2) for c in live(sd, lo + 1)]
        new_cells = [] if final else [(sd, c) for sd in range(2) for c in live(sd, lo + 2)]

        def halo_rolls():
            for sd, c in lap_cells:
                hv[sd, c] = vertical(qh, sd, c)

        def halo_lap():
            for sd, c in lap_cells:
                for half in range(2):
                    nxt, prv = hv[sd, c][half]
                    xm, xp = halo_x(qh, acc_in, sd, c, half)
                    lap = (nxt + prv) + (xp + xm) - 4.0 * qh(sd, c, half)
                    LH[sd, c, half] = jnp.where(edge_ok[sd], lap, 0.0)
                    if (sd, c) in new_cells:
                        grads[sd, c, half] = (UH[sd, c, half, 0:1] * (xp - xm) + UH[sd, c, half, 1:2] * (nxt - prv))

        def lap_rolls():
            for sd, c in new_cells:
                lv[sd, c] = vertical(lh, sd, c)

        def halo_new():
            for sd, c in new_cells:
                for half in range(2):
                    nxt, prv = lv[sd, c][half]
                    xm, xp = halo_x(lh, acc_l, sd, c, half)
                    mid = lh(sd, c, half)
                    around = (nxt + prv) + (xp + xm)
                    new = (keep * qh(sd, c, half) + (FH[sd, c, half] - grads[sd, c, half])
                           + (lap_gain * mid - hyper * around))
                    H[dst, sd, c, half] = new * UH[sd, c, half, 2:3]

        def turn_first(i):
            turn1[i] = across(Q[src, i, 0], Q[src, i, 7], qh, i)

        def first_pass(i):
            left, right = turn1.pop(i)
            row = [Q[src, i, c] for c in range(8)]
            laps = []
            for c in range(8):
                xm = row[c - 1] if c else left
                xp = row[c + 1] if c < 7 else right
                up_, dn = Q[src, i + 1, c], Q[src, i - 1, c]
                laps.append(masked(i, (up_ + dn) + (xp + xm) - 4.0 * row[c]))
                L[i, c] = laps[c]
                if lo + 2 <= i < hi - 2:
                    a = US[0, c, i:i + 1, :] * (xp - xm) + US[1, c, i:i + 1, :] * (up_ - dn)
                    adv[i, c] = keep * row[c] + (FO[i, c] - a)
            if not final:
                inward(acc_l, i, laps[0], laps[7])
            if lo + 2 <= i < hi - 2:
                turn2[i] = across(laps[0], laps[7], lh, i)

        def second_pass(i):
            left, right = turn2.pop(i)
            row = [L[i, c] for c in range(8)]
            outs = []
            for c in range(8):
                xm = row[c - 1] if c else left
                xp = row[c + 1] if c < 7 else right
                around = (L[i + 1, c] + L[i - 1, c]) + (xp + xm)
                new = (adv.pop((i, c)) + (lap_gain * row[c] - hyper * around)) * US[2, c, i:i + 1, :]
                outs.append(new)
                if not final:
                    Q[dst, i, c] = new
            if not final:
                inward(acc_out, i, outs[0], outs[7])
                return
            ys = skew(outs)

            def middle():
                xs = unskew(ys)

                def end():
                    r = i - DEPTH
                    ref = flat(out_lo if r < DEPTH else out_hi)
                    for v, x in enumerate(xs):
                        ref[pl.ds(v * 8 * DEPTH + r % DEPTH, 8, stride=DEPTH), :] = x
                at_slot(slot[0] + LAT, end)
            at_slot(slot[0] + LAT, middle)

        halo_rolls()
        for k in range(LAT):
            turn_first(lo + 1 + k)
        while any(fn.__name__ == "put" for fns in queue.values() for fn in fns):
            tick()
        halo_lap()
        lap_rolls()
        for i in range(lo + 1, hi - 1):
            if i + LAT < hi - 1:
                turn_first(i + LAT)
            first_pass(i)
            if lo + 2 <= i < hi - 2:
                at_slot(slot[0] + LAT, functools.partial(second_pass, i))
            tick()
        for _ in range(LAT):
            tick()
        if not final:
            halo_new()
        return acc_out

    acc = acc_q
    for s in range(STEPS):
        acc = advance(s, acc)
    drain()

    index = index_ref[0]
    col = jnp.bitwise_and(index, cols - 1)
    row = jnp.right_shift(index, cols.bit_length() - 1)
    hot = (lax.broadcasted_iota(I32, (cols, cols), 0) == col).astype(jnp.bfloat16)
    row_id = lax.broadcasted_iota(I32, (8, DEPTH, cols), 1)
    dot = functools.partial(jnp.dot, preferred_element_type=F32)
    for g in range(members // 8):
        found = []
        for h, ref in ((0, out_lo), (rows - DEPTH, out_hi)):
            x = flat(ref)[pl.ds(g * 8 * DEPTH, 8 * DEPTH), :]
            x1 = x.astype(jnp.bfloat16)
            rem = x - x1.astype(F32)
            x2 = rem.astype(jnp.bfloat16)
            x3 = (rem - x2.astype(F32)).astype(jnp.bfloat16)
            picked = dot(x1, hot) + (dot(x2, hot) + dot(x3, hot))
            found.append(jnp.where(row_id + h == row[None], picked.reshape(8, DEPTH, cols), 0.0))
        obs_ref[pl.ds(g * 8, 8), :] = jnp.sum(found[0] + found[1], axis=1)
        for h, c in obs_copies:
            if (g + 1) * 8 == (early, members)[h]:
                c.start()

    obs_all[mine, :] = obs_ref[...]
    th_ref[ens] = theta_ref[...]
    for _, c in obs_copies:
        c.wait()

    x = obs_all[...]
    mean = jnp.mean(x, axis=0, keepdims=True)
    inv = 1.0 / sig_ref[0]
    anom = (x - mean) * inv
    d = jnp.broadcast_to((val_ref[0] - mean) * inv, (8, x.shape[1]))
    total = x.shape[0]
    gram = lax.dot_general(jnp.concatenate([anom, d], axis=0), anom, (((1,), (1,)), ((), ())),
                           preferred_element_type=F32, precision=HIGH)

    def finish():
        for c in (to_right, to_left):
            c.wait_send()
        for ok, copies in ((has_down, fall + downs), (has_up, rise + ups)):
            @pl.when(ok)
            def _():
                for c in copies:
                    c.wait_send()
        for c in th_copies:
            c.wait()

    if not reduce_here:
        for k, piece in enumerate(fold(gram, total)):
            full_ref[8 * k:8 * k + 8, :] = piece
        finish()
        return
    for k, piece in enumerate(fold(gram, total)):
        part[8 * k:8 * k + 8, :] = piece
    spans = share(folded(total), len(owners))
    rank = [oy * n_gx + ox for ox, oy in owners]

    def to_owner(k, slot_):
        return rdma(part.at[spans[k]], rs.at[slot_, 0:spans[k].size], rs_send.at[k], rs_recv.at[0],
                    {"gx": owners[k][0], "gy": owners[k][1]})

    def all_slots(k):
        return rs.at[:, 0:spans[k].size]

    def arrivals(k):
        return rdma(all_slots(k), all_slots(k), rs_send.at[k], rs_recv.at[0],
                    {"gx": owners[k][0], "gy": owners[k][1]})

    def departures(k):
        return rdma(all_slots(k), all_slots(k), ag_send.at[0], ag_recv.at[k], where[0])

    def from_owner(k, j):
        return rdma(full_ref.at[spans[k]], full_ref.at[spans[k]], ag_send.at[0], ag_recv.at[k], where[j])

    for k in range(len(owners)):
        @pl.when(me != rank[k])
        def _():
            to_owner(k, lax.rem(me + (n - 1 - rank[k]), n)).start()
    for k in range(len(owners)):
        @pl.when(me == rank[k])
        def _():
            arrivals(k).wait_recv()
            terms = [part[spans[k], :]] + [rs[p, 0:spans[k].size, :] for p in range(n - 1)]
            while len(terms) > 1:
                terms = [sum(terms[t:t + 2][1:], terms[t]) for t in range(0, len(terms), 2)]
            full_ref[spans[k], :] = terms[0]
            for j in range(len(where)):
                from_owner(k, j).start()
    for k in range(len(owners)):
        @pl.when(me != rank[k])
        def _():
            to_owner(k, 0).wait_send()
    finish()
    for k in range(len(owners)):
        @pl.when(me != rank[k])
        def _():
            from_owner(k, 0).wait_recv()

        @pl.when(me == rank[k])
        def _():
            departures(k).wait_send()


def run_step(mesh, state, forcing, u_vel, v_vel, land, member_mode, theta, obs_index, values, sigma):
    n_gx, n_gy, n_ens = mesh.shape["gx"], mesh.shape["gy"], mesh.shape["ens"]
    members, rows, cols = state.shape
    patterns = forcing.shape[0]
    sites = obs_index.shape[-1]
    params = theta.shape[1]
    nf = -(-(patterns + 3) // 8) * 8
    strips = members + nf
    n_rows = rows + 2 * DEPTH
    total = members * n_ens
    n = n_gx * n_gy
    owners = [(ox, oy) for oy in range(1, n_gy, 2) for ox in sorted({max(n_gx // 2 - 1, 0), n_gx // 2})]
    reduce_here = n <= 32 and len(owners) > 0
    own = max(p.size for p in share(folded(total), len(owners))) if reduce_here else 8
    slots = n - 1 if reduce_here else 1
    sums = len(owners) if reduce_here else 1
    sds = jax.ShapeDtypeStruct
    dma = pltpu.SemaphoreType.DMA
    reg = (8, cols)
    out_lo, out_hi, full, th = pl.pallas_call(
        functools.partial(step_kernel, n_gx, n_gy, n_ens, reduce_here, owners),
        out_shape=[sds((members, DEPTH, cols), F32)] * 2 + [sds((folded(total), total), F32),
                   sds((n_ens, params, members), F32)],
        in_specs=[hspec()] * 10,
        out_specs=[vspec()] * 4,
        scratch_shapes=[VM((members, DEPTH, cols), F32)] * 2 + [VM((nf, DEPTH, cols), F32)] * 2
        + [VM((rows, cols), I32), VM((1, members), I32), VM((params, members), F32), VM((1, 1, sites), I32),
           VM((1, 1, sites), F32), VM((1, 1, sites), F32)]
        + [VM((members, DEPTH, cols), F32)] * 2 + [VM((nf, DEPTH, cols), F32)] * 2
        + [VM((2, strips, cols), F32), VM((2, 2, strips // 2, cols), F32), VM((2, strips, cols), F32)]
        + [VM((2, strips // 2, cols), F32)] * 2
        + [VM((2, n_rows, 8) + reg, F32), VM((n_rows, 8) + reg, F32), VM((n_rows, 8) + reg, F32),
           VM((3, 8, n_rows, cols), F32),
           VM((2, 2, 8, 2) + reg, F32), VM((2, 8, 2) + reg, F32), VM((2, 8, 2) + reg, F32),
           VM((2, 8, 2) + reg, F32), VM(reg, F32)]
        + [VM((members, sites), F32), VM((total, sites), F32), VM((folded(total), total), F32), VM((slots, own, total), F32)]
        + [dma((14,)), dma((6,)), dma((6,)), dma((2,)), dma((2,)), dma((4,)), dma((4,))]
        + [dma((3 * (n_ens - 1),))] * 2 + [dma((sums,)), dma((1,)), dma((1,)), dma((sums,))],
        compiler_params=pltpu.CompilerParams(collective_id=0, has_side_effects=True, vmem_limit_bytes=SPACE),
        name="step",
    )(*[pltpu.with_memory_space_constraint(x, pltpu.HBM) for x in
        (state, forcing, u_vel, v_vel, land, member_mode.reshape(1, members), theta.T, obs_index, values, sigma)])
    if not reduce_here:
        full = lax.psum(full, ("gx", "gy"))
    return out_lo, out_hi, full, th


def solve_kernel(members, full_ref, th_ref, out_ref, xs):
    total = full_ref.shape[1]
    blocks = total // 8
    n_ens, params = th_ref.shape[0], th_ref.shape[1]
    shape = (8, total)
    lane = lax.broadcasted_iota(jnp.int32, shape, 1)
    sub = lax.broadcasted_iota(jnp.int32, shape, 0)
    tht = jnp.concatenate([th_ref[e] for e in range(n_ens)], axis=1)
    spread = tht - jnp.mean(tht, axis=1, keepdims=True)
    xs[...] = jnp.zeros_like(xs)
    xs[0:params, :] = spread
    cols_of = xs[...].T
    A, R = [], []
    gram = unfold(full_ref, total)
    for k in range(blocks):
        rows = slice(8 * k, 8 * k + 8)
        A.append(gram[k] + jnp.where(lane == sub + 8 * k, float(total - 1), 0.0))
        R.append(cols_of[rows])

    def splat(x):
        return jnp.broadcast_to(x, shape)

    def columns(x, k):
        return [jnp.take_along_axis(x, jnp.full(shape, 8 * k + j, jnp.int32), axis=1, mode="promise_in_bounds")
                for j in range(8)]

    def less(x, terms):
        terms = list(terms)
        while len(terms) > 1:
            terms = [sum(terms[t:t + 2][1:], terms[t]) for t in range(0, len(terms), 2)]
        return x - terms[0]

    for k in range(blocks):
        cols_k = columns(A[k], k)
        d = {(j, i): splat(cols_k[i][j:j + 1]) for j in range(8) for i in range(j, 8)}
        sets = [[splat(A[k][j:j + 1]) for j in range(8)]]
        if k == 0:
            sets.append([splat(R[k][j:j + 1]) for j in range(8)])
        pairs = {}
        for p in range(0, 8, 2):
            a, b, c = d[p, p], d[p, p + 1], d[p + 1, p + 1]
            r = 1.0 / (a * c - b * b)
            pairs[p] = a * r, b * r, c * r
            for i in range(p + 2, 8):
                m0 = (d[p, i] * c - d[p + 1, i] * b) * r
                m1 = (d[p + 1, i] * a - d[p, i] * b) * r
                for rs_ in sets:
                    rs_[i] = rs_[i] - (m0 * rs_[p] + m1 * rs_[p + 1])
                for q in range(i, 8):
                    d[i, q] = d[i, q] - (m0 * d[p, q] + m1 * d[p + 1, q])
        for p in reversed(range(0, 8, 2)):
            ar, br, cr = pairs[p]
            for rs_ in sets:
                y0, y1 = rs_[p], rs_[p + 1]
                if p < 6:
                    y0 = less(y0, [d[p, j] * rs_[j] for j in range(p + 2, 8)])
                    y1 = less(y1, [d[p + 1, j] * rs_[j] for j in range(p + 2, 8)])
                rs_[p], rs_[p + 1] = cr * y0 - br * y1, ar * y1 - br * y0

        def merge(rs_):
            x = rs_[7]
            for j in range(7):
                x = jnp.where(sub == j, rs_[j], x)
            return x

        for i in list(range(k + 1, blocks)) + list(range(k)):
            c = columns(A[i], k)
            A[i] = less(A[i], [c[j] * sets[0][j] for j in range(8)])
            if k == 0:
                R[i] = less(R[i], [c[j] * sets[1][j] for j in range(8)])
                A[i] = jnp.where(lane < 8, R[i], A[i])
        A[k] = merge(sets[0])
        if k == 0:
            A[k] = jnp.where(lane < 8, merge(sets[1]), A[k])
    for k in range(blocks):
        xs[8 * k:8 * k + 8, :] = A[k]
    x = xs[...].T[0:8]
    shift = jnp.sum(x * full_ref[folded(total) - 8:folded(total) - 7, :], axis=1, keepdims=True)
    new = (jnp.mean(tht, axis=1, keepdims=True) + shift[0:params]) + float(total - 1) * x[0:params]
    ens = lax.axis_index("ens")
    for e in range(n_ens):
        @pl.when(ens == e)
        def _():
            out_ref[...] = new[:, e * members:(e + 1) * members]


def relay_kernel(members, full_ref, th_ref, lo_ref, hi_ref, out_ref, final_ref, xs, sem):
    depth, rows = lo_ref.shape[1], final_ref.shape[1]
    gives = [pltpu.make_async_copy(lo_ref, final_ref.at[:, 0:depth, :], sem.at[0]),
             pltpu.make_async_copy(hi_ref, final_ref.at[:, rows - depth:, :], sem.at[1])]
    for c in gives:
        c.start()
    solve_kernel(members, full_ref, th_ref, out_ref, xs)
    for c in gives:
        c.wait()


def solve(full, th, theta, lo, hi, shape):
    total = full.shape[1]
    out, final = pl.pallas_call(
        functools.partial(relay_kernel, theta.shape[0]),
        out_shape=[jax.ShapeDtypeStruct(theta.shape[::-1], F32), jax.ShapeDtypeStruct(shape, F32)],
        in_specs=[vspec()] * 4,
        out_specs=[vspec(), hspec()],
        scratch_shapes=[VM((total, total), F32), pltpu.SemaphoreType.DMA((2,))],
        compiler_params=pltpu.CompilerParams(vmem_limit_bytes=SMALL_SPACE),
        name="solve",
    )(full, th, lo, hi)
    return out.T, final


def local(mesh, state, u_vel, v_vel, land, forcing, member_mode, theta, obs_index, obs_values, obs_sigma):
    lo, hi, full, th = run_step(mesh, state, forcing, u_vel, v_vel, land, member_mode, theta, obs_index,
                                obs_values, obs_sigma)
    new_theta, final = solve(full, th, theta, lo, hi, state.shape)
    return final, new_theta


def solution(mesh):
    placed = (
        P("ens", "gy", "gx"),
        P("gy", "gx"),
        P("gy", "gx"),
        P("gy", "gx"),
        P(None, "gy", "gx"),
        P("ens"),
        P("ens", None),
        P("gy", "gx", None),
        P("gy", "gx", None),
        P("gy", "gx", None),
    )
    return jax.shard_map(
        functools.partial(local, mesh),
        mesh=mesh,
        in_specs=placed,
        out_specs=(P("ens", "gy", "gx"), P("ens", None)),
        check_vma=False,
    )
```
